512 devices in a mesh: group: 16 (over y, core), dom: 32 (over x, z).
Axes of the slice: x: 4, y: 8, z: 8, core: 2. Of those that a mesh axis runs over, the one named last changes fastest.
Arguments:
- hidden: bfloat16 [524288, 512], P(('group', 'dom')), may hold values from -6 to 6
- enc_weight: bfloat16 [512, 512], replicated, may hold values from -0.25 to 0.25
- enc_bias: float32 [512], replicated, may hold values from -3 to 3
- enc_slope: float32 [512], replicated, may hold values from 0.05 to 0.5
- dec_token: bfloat16 [512], replicated, may hold values from -4 to 4
- dec_weight: bfloat16 [512, 128], replicated, may hold values from -0.25 to 0.25
- dec_bias: float32 [128], replicated, may hold values from -3 to 3
- targets: bfloat16 [524288, 128], P(('group', 'dom')), may hold values from -6 to 6
- local_tiles: bfloat16 [6144, 128, 128], P(('group', 'dom')), may hold values from -0.375 to 0.375
- local_src: int32 [512, 12], P(('group', 'dom')), may hold values from 0 to 7
- local_dst: int32 [512, 12], P(('group', 'dom')), may hold values from 0 to 7
- local_count: int32 [512], P(('group', 'dom')), may hold values from 4 to 12, as said below
- halo_tiles: bfloat16 [4096, 128, 128], P(('group', 'dom')), may hold values from -0.375 to 0.375
- halo_src: int32 [512, 8], P(('group', 'dom')), may hold values from 0 to 7, each once within a row
- halo_dst: int32 [512, 8], P(('group', 'dom')), may hold values from 0 to 7
- send_rows: int32 [16384, 16], P(('group', 'dom')), may hold values from 0 to 1023
- cross_rows: int32 [8192, 32], P(('group', 'dom')), may hold values from 0 to 1023
- mask_nodes: int32 [512, 512], P(('group', 'dom')), may hold values from 0 to 1023, as said below
- remask_nodes: int32 [512, 256], P(('group', 'dom')), may hold values from 0 to 1023, as said below
Outputs:
- rebuilt: bfloat16 [524288, 128], P(('group', 'dom'))
- node_error: float32 [524288], P(('group', 'dom'))
The draws below stay inside these ranges and needn't reach their ends.
Inputs may be any that keep to these rules, and one draw needn't show every extreme that they name: `local_count`: live local tiles of a partition; tile slots at or past it are ignored; some partition has 12. `halo_src`: each partition's row names each of its boundary blocks once. `mask_nodes`: distinct rows within a partition. `remask_nodes`: distinct rows within a partition.
All inputs are finite; a program needn't handle non-finite values.
Results may differ from the reference program's by a relative error of at most 0.0056.
Values may be sent and summed in bfloat16 or wider, within the bound.
A program may use at most 64 MiB of HBM per device.

```python
import math
import jax
import jax.numpy as jnp
from jax import lax

D_HID = 512
D_FEAT = 128
BLK = 128
ROWS_DEV = 1024
NODES = 524288
HALO_DOM = 512
HALO_GRP = 512
HALO_BLOCKS = 8
LOCAL_TILES = 12
MASK_DEV = 512
REMASK_DEV = 256
N_GROUP = 16
N_DOM = 32


def pick_rows(key, chosen):
    device_keys = jax.random.split(key, N_GROUP * N_DOM)

    def shuffle(seed_key):
        return jax.random.permutation(seed_key, ROWS_DEV)
    orders = jax.vmap(shuffle)(device_keys)
    return orders[:, :chosen].astype(jnp.int32)


def draw_mask_nodes(key, part):
    return pick_rows(jax.random.fold_in(key, 11), MASK_DEV)


def draw_remask_nodes(key, part):
    return pick_rows(jax.random.fold_in(key, 23), REMASK_DEV)


def draw_local_count(key, part):
    devices = N_GROUP * N_DOM
    counts = jax.random.randint(jax.random.fold_in(key, 5), (devices,), LOCAL_TILES // 3, LOCAL_TILES + 1)
    spot = jax.random.randint(jax.random.fold_in(key, 7), (), 0, devices)
    return counts.at[spot].set(LOCAL_TILES).astype(jnp.int32)


def plant(result, own_key, smallest, high):
    dims = result.shape
    place = [jax.random.randint(jax.random.fold_in(own_key, axis), (), 0, dims[axis]) for axis in range(len(dims))]
    result = result.at[tuple(place)].set(smallest)
    longest = dims.index(max(dims))
    place[longest] = (place[longest] + 1) % dims[longest]
    return result.at[tuple(place)].set(high)


def shard_levels(rng, dims, cuts, low, top_value):
    factor_of = 1.0
    for dim, blocks in cuts:
        draws = jax.random.uniform(jax.random.fold_in(jax.random.fold_in(rng, 6), dim), (blocks,), jnp.float32, low / len(cuts), top_value / len(cuts))
        factor_of = factor_of * jnp.repeat(jnp.exp(draws), dims[dim] // blocks).reshape((-1,) + (1,) * (len(dims) - 1 - dim))
    return factor_of


def scatter_about(stream_key, shape, scale, bound, cuts=(), kind=jnp.bfloat16):
    level = shard_levels(stream_key, shape, cuts, -0.22, 0.18) if cuts else 1.0
    values = jax.random.normal(stream_key, shape, jnp.float32) * scale * level
    return jnp.minimum(jnp.maximum(values, -bound), bound).astype(kind)


def setup_inputs(seed: int = 0) -> dict:
    keys = jax.random.split(jax.random.key(seed), 20)
    hidden = scatter_about(keys[0], (NODES, D_HID), 1.0, 6.0, ((0, 512),))
    enc_weight = scatter_about(keys[1], (D_HID, D_HID), D_HID ** -0.5, 0.25)
    enc_bias = scatter_about(keys[2], (D_HID,), 0.5, 3.0, (), jnp.float32)
    enc_slope = jnp.clip(jnp.exp(jax.random.uniform(keys[3], (D_HID,), jnp.float32, math.log(0.05), math.log(0.5))), 0.05, 0.5)
    dec_token = scatter_about(keys[4], (D_HID,), 1.0, 4.0)
    dec_weight = scatter_about(keys[5], (D_HID, D_FEAT), D_HID ** -0.5, 0.25)
    dec_bias = scatter_about(keys[6], (D_FEAT,), 0.5, 3.0, (), jnp.float32)
    targets = scatter_about(keys[7], (NODES, D_FEAT), 1.0, 6.0, ((0, 512),))
    local_tiles = scatter_about(keys[8], (N_GROUP * N_DOM * LOCAL_TILES, BLK, BLK), (2 * BLK) ** -0.5, 0.375, ((0, 512),))
    local_src = plant(jax.random.randint(keys[9], (N_GROUP * N_DOM, LOCAL_TILES), 0, ROWS_DEV // BLK), jax.random.fold_in(keys[9], 1), 0, (ROWS_DEV // BLK) - 1).astype(jnp.int32)
    local_dst = plant(jax.random.randint(keys[10], (N_GROUP * N_DOM, LOCAL_TILES), 0, ROWS_DEV // BLK), jax.random.fold_in(keys[10], 1), 0, (ROWS_DEV // BLK) - 1).astype(jnp.int32)
    local_count = draw_local_count(jax.random.fold_in(keys[19], 71), 0)
    halo_tiles = scatter_about(keys[12], (N_GROUP * N_DOM * HALO_BLOCKS, BLK, BLK), (2 * BLK) ** -0.5, 0.375, ((0, 512),))
    halo_src = jax.vmap(lambda own: jax.random.permutation(own, HALO_BLOCKS))(jax.random.split(keys[13], (N_GROUP * N_DOM))).reshape((N_GROUP * N_DOM, HALO_BLOCKS)).astype(jnp.int32)
    halo_dst = plant(jax.random.randint(keys[14], (N_GROUP * N_DOM, HALO_BLOCKS), 0, ROWS_DEV // BLK), jax.random.fold_in(keys[14], 1), 0, (ROWS_DEV // BLK) - 1).astype(jnp.int32)
    send_rows = plant(jax.random.randint(keys[15], (N_GROUP * N_DOM * N_DOM, HALO_DOM // N_DOM), 0, ROWS_DEV), jax.random.fold_in(keys[15], 1), 0, ROWS_DEV - 1).astype(jnp.int32)
    cross_rows = plant(jax.random.randint(keys[16], (N_GROUP * N_DOM * N_GROUP, HALO_GRP // N_GROUP), 0, ROWS_DEV), jax.random.fold_in(keys[16], 1), 0, ROWS_DEV - 1).astype(jnp.int32)
    mask_nodes = draw_mask_nodes(jax.random.fold_in(keys[19], 71), 0)
    remask_nodes = draw_remask_nodes(jax.random.fold_in(keys[19], 71), 0)
    return dict(hidden=hidden, enc_weight=enc_weight, enc_bias=enc_bias, enc_slope=enc_slope, dec_token=dec_token, dec_weight=dec_weight, dec_bias=dec_bias, targets=targets, local_tiles=local_tiles, local_src=local_src, local_dst=local_dst, local_count=local_count, halo_tiles=halo_tiles, halo_src=halo_src, halo_dst=halo_dst, send_rows=send_rows, cross_rows=cross_rows, mask_nodes=mask_nodes, remask_nodes=remask_nodes)


def project(inputs, weight):
    return jnp.dot(inputs, weight, preferred_element_type=jnp.float32).astype(jnp.bfloat16)

def halo_index(send_rows, cross_rows):
    groups = N_GROUP
    domains = N_DOM
    per_dom = HALO_DOM // domains
    per_group = HALO_GRP // groups
    group_ids = jnp.arange(groups, dtype=jnp.int32)
    domain_ids = jnp.arange(domains, dtype=jnp.int32)
    row_base = (group_ids[:, None] * domains + domain_ids[None, :]) * ROWS_DEV
    sent_rows = send_rows.astype(jnp.int32).reshape(groups, domains, domains, per_dom)
    dom_index = row_base[:, :, None, None] + sent_rows
    dom_index = jnp.transpose(dom_index, (0, 2, 1, 3)).reshape(groups * domains, HALO_DOM)
    cross_list = cross_rows.astype(jnp.int32).reshape(groups, domains, groups, per_group)
    group_index = row_base[:, :, None, None] + cross_list
    group_index = jnp.transpose(group_index, (2, 1, 0, 3)).reshape(groups * domains, HALO_GRP)
    return jnp.concatenate([dom_index, group_index], axis=1).astype(jnp.int32)

def spread(tile_values, sources, targets, live_tiles, source_pool):
    picked = source_pool[sources].astype(jnp.float32)
    partial_terms = jnp.einsum('tij,tjf->tif', tile_values.astype(jnp.float32), picked, precision=lax.Precision.HIGHEST)
    blocks = ROWS_DEV // BLK
    onehot = ((targets[None, :] == jnp.arange(blocks, dtype=jnp.int32)[:, None]) & live_tiles[None, :]).astype(jnp.float32)
    summed = jnp.einsum('nt,tif->nif', onehot, partial_terms, precision=lax.Precision.HIGHEST)
    return summed.reshape(ROWS_DEV, -1)

def propagate(features, halo_rows, local_tiles, local_src, local_dst, local_count, halo_tiles, halo_src, halo_dst):
    width = features.shape[1]
    blocks = ROWS_DEV // BLK

    def one_device(device):
        own_rows = lax.dynamic_slice_in_dim(features, device * ROWS_DEV, ROWS_DEV, 0)
        remote = features[halo_rows[device]]
        source_pool = jnp.concatenate([own_rows, remote], axis=0).reshape(-1, BLK, width)
        local_values = lax.dynamic_slice_in_dim(local_tiles, device * LOCAL_TILES, LOCAL_TILES, 0)
        remote_values = lax.dynamic_slice_in_dim(halo_tiles, device * HALO_BLOCKS, HALO_BLOCKS, 0)
        live_tiles = jnp.arange(LOCAL_TILES, dtype=jnp.int32) < local_count[device]
        every_tile = jnp.ones((HALO_BLOCKS,), dtype=jnp.bool_)
        inner = spread(local_values, local_src[device], local_dst[device], live_tiles, source_pool)
        outer = spread(remote_values, halo_src[device] + blocks, halo_dst[device], every_tile, source_pool)
        return inner + outer
    devices = jnp.arange(N_GROUP * N_DOM, dtype=jnp.int32)
    return lax.map(one_device, devices).reshape(-1, width)

def reference(hidden, enc_weight, enc_bias, enc_slope, dec_token, dec_weight, dec_bias, targets, local_tiles, local_src, local_dst, local_count, halo_tiles, halo_src, halo_dst, send_rows, cross_rows, mask_nodes, remask_nodes):
    halo_rows = halo_index(send_rows, cross_rows)
    encoded = project(hidden, enc_weight)
    summed = propagate(encoded, halo_rows, local_tiles, local_src, local_dst, local_count, halo_tiles, halo_src, halo_dst) + enc_bias[None, :]
    latent = jnp.where(summed > 0, summed, enc_slope[None, :] * summed).astype(jnp.bfloat16)
    offsets = (jnp.arange(N_GROUP * N_DOM, dtype=jnp.int32) * ROWS_DEV)[:, None]
    node_total = N_GROUP * N_DOM * ROWS_DEV
    remasked = jnp.zeros((node_total,), jnp.bool_).at[(offsets + remask_nodes.astype(jnp.int32)).reshape(-1)].set(True)
    masked = jnp.zeros((node_total,), jnp.bool_).at[(offsets + mask_nodes.astype(jnp.int32)).reshape(-1)].set(True)
    decoder_in = jnp.where(remasked[:, None], dec_token[None, :], latent)
    narrowed = project(decoder_in, dec_weight)
    decoded = propagate(narrowed, halo_rows, local_tiles, local_src, local_dst, local_count, halo_tiles, halo_src, halo_dst) + dec_bias[None, :]
    rebuilt = decoded.astype(jnp.bfloat16)
    values = rebuilt.astype(jnp.float32)
    target_values = targets.astype(jnp.float32)
    cosine = lax.optimization_barrier(jnp.mean(values * target_values, axis=1)) * lax.rsqrt(lax.optimization_barrier(jnp.mean(values * values, axis=1)) + 1e-06) * lax.rsqrt(lax.optimization_barrier(jnp.mean(target_values * target_values, axis=1)) + 1e-06)
    node_error = jnp.where(masked, (1.0 - cosine) ** 2, jnp.zeros_like(cosine))
    return (rebuilt, node_error)
```

```python
import jax
import jax.numpy as jnp
from jax import lax
from jax.experimental import pallas as pl
from jax.experimental.pallas import tpu as pltpu
from jax.sharding import PartitionSpec as P

BLK = 128
F32 = jnp.float32
BF16 = jnp.bfloat16
I32 = jnp.int32
Z_ORDER = (4, 3, 5, 2, 6, 1, 7, 0)
G_ORDER = (0, 1, 2, 3)


def iota(shape, axis):
    return lax.broadcasted_iota(I32, shape, axis)


def step_kernel(
    hidden,
    enc_weight,
    enc_bias,
    enc_slope,
    dec_token,
    dec_weight,
    dec_bias,
    targets,
    local_tiles,
    local_src,
    local_dst,
    local_count,
    halo_tiles,
    halo_src,
    halo_dst,
    send_index,
    mask_nodes,
    remask_nodes,
    rebuilt,
    node_error,
    hid_v,
    encw_v,
    decw_v,
    tgt_v,
    lt_v,
    ht_v,
    enc,
    onehot,
    out_wide,
    in_wide,
    acc,
    remasked,
    masked,
    narrowed,
    out_thin,
    in_thin,
    acc_thin,
    load_sem,
    send_wide,
    recv_wide,
    send_thin,
    recv_thin,
):
    mg = lax.axis_index("group")
    md = lax.axis_index("dom")
    mx = md // 8
    mz = md % 8
    mq = mg // 4

    barrier = pltpu.get_barrier_semaphore()

    def greet_dom(k, carry):
        pl.semaphore_signal(
            barrier, inc=1, device_id=(mg, (md + k) % 32), device_id_type=pl.DeviceIdType.MESH
        )
        return carry

    def greet_group(k, carry):
        pl.semaphore_signal(
            barrier, inc=1, device_id=((mg + k) % 16, md), device_id_type=pl.DeviceIdType.MESH
        )
        return carry

    lax.fori_loop(1, 32, greet_dom, 0)
    lax.fori_loop(1, 16, greet_group, 0)

    loads = [
        pltpu.make_async_copy(src, dst, load_sem.at[k])
        for k, (src, dst) in enumerate(
            (
                (hidden, hid_v),
                (enc_weight, encw_v),
                (local_tiles, lt_v),
                (halo_tiles, ht_v),
                (dec_weight, decw_v),
                (targets, tgt_v),
            )
        )
    ]
    for load in loads:
        load.start()

    def build_onehot(b, carry):
        row = jnp.broadcast_to(send_index[pl.ds(b, 1), :], (BLK, BLK))
        column = jnp.transpose(row)
        for j in range(8):
            hit = column == iota((BLK, BLK), 1) + j * BLK
            onehot[b, :, j * BLK : (j + 1) * BLK] = jnp.where(hit, 1.0, 0.0).astype(BF16)
        return carry

    lax.fori_loop(0, 8, build_onehot, 0)

    loads[0].wait()
    loads[1].wait()

    def encode(c, carry):
        rows = hid_v[pl.ds(c * 2, 2)].reshape(2 * BLK, 512)
        made = jnp.dot(rows, encw_v[...], preferred_element_type=F32).astype(BF16)
        enc[pl.ds(c * 2, 2)] = made.reshape(2, BLK, 512)
        return carry

    lax.fori_loop(0, 4, encode, 0)

    pl.semaphore_wait(barrier, 46)

    def wide_dom(x, z):
        return pltpu.make_async_remote_copy(
            src_ref=out_wide.at[x, pl.ds(z * 16, 16)],
            dst_ref=in_wide.at[mx, pl.ds(mz * 16, 16)],
            send_sem=send_wide.at[x * 8 + z],
            recv_sem=recv_wide.at[md],
            device_id=(mg, x * 8 + z),
            device_id_type=pl.DeviceIdType.MESH,
        )

    def wide_group(q, r):
        return pltpu.make_async_remote_copy(
            src_ref=out_wide.at[4 + q, pl.ds(r * 32, 32)],
            dst_ref=in_wide.at[4 + mq, pl.ds((mg % 4) * 32, 32)],
            send_sem=send_wide.at[32 + q * 4 + r],
            recv_sem=recv_wide.at[32 + mg],
            device_id=(q * 4 + r, md),
            device_id_type=pl.DeviceIdType.MESH,
        )

    def thin_dom(x, z):
        return pltpu.make_async_remote_copy(
            src_ref=out_thin.at[x, pl.ds(z * 16, 16)],
            dst_ref=in_thin.at[mx, pl.ds(mz * 16, 16)],
            send_sem=send_thin.at[x * 8 + z],
            recv_sem=recv_thin.at[md],
            device_id=(mg, x * 8 + z),
            device_id_type=pl.DeviceIdType.MESH,
        )

    def thin_group(q, r):
        return pltpu.make_async_remote_copy(
            src_ref=out_thin.at[4 + q, pl.ds(r * 32, 32)],
            dst_ref=in_thin.at[4 + mq, pl.ds((mg % 4) * 32, 32)],
            send_sem=send_thin.at[32 + q * 4 + r],
            recv_sem=recv_thin.at[32 + mg],
            device_id=(q * 4 + r, md),
            device_id_type=pl.DeviceIdType.MESH,
        )

    def push(x, q, dom_copy, group_copy):
        for k in range(4):
            for z_step in Z_ORDER[2 * k : 2 * k + 2]:
                z = (mz + z_step) % 8

                @pl.when(x * 8 + z != md)
                def _():
                    dom_copy(x, z).start()

            r = (mg + G_ORDER[k]) % 4

            @pl.when(q * 4 + r != mg)
            def _():
                group_copy(q, r).start()

    def gather_send(source, width, out_ref, dom_copy, group_copy):
        def chunk(c, carry):
            off = jnp.where(c == 0, 2, jnp.where(c == 1, 1, jnp.where(c == 2, 3, 0)))
            x = (mx + off) % 4
            q = (mq + off) % 4
            chosen = jnp.concatenate([onehot[x], onehot[4 + q]], axis=0)
            rows = jnp.dot(chosen, source[...].reshape(1024, width), preferred_element_type=F32)
            rows = rows.astype(BF16)
            out_ref[x] = rows[:BLK]
            out_ref[4 + q] = rows[BLK:]
            push(x, q, dom_copy, group_copy)
            return carry

        lax.fori_loop(0, 4, chunk, 0)

    def keep_own(out_ref, in_ref):
        in_ref[mx, pl.ds(pl.multiple_of(mz * 16, 16), 16)] = out_ref[
            mx, pl.ds(pl.multiple_of(mz * 16, 16), 16)
        ]
        own = pl.multiple_of((mg % 4) * 32, 32)
        in_ref[4 + mq, pl.ds(own, 32)] = out_ref[4 + mq, pl.ds(own, 32)]

    def wait_dom(x, in_ref, send, recv):
        def one(z, carry):
            @pl.when(x * 8 + z != md)
            def _():
                part = in_ref.at[x, pl.ds(z * 16, 16)]
                pltpu.make_async_remote_copy(
                    src_ref=part,
                    dst_ref=part,
                    send_sem=send.at[x * 8 + z],
                    recv_sem=recv.at[x * 8 + z],
                    device_id=(mg, x * 8 + z),
                    device_id_type=pl.DeviceIdType.MESH,
                ).wait_recv()

            return carry

        lax.fori_loop(0, 8, one, 0)

    def wait_group(q, in_ref, send, recv):
        def one(r, carry):
            @pl.when(q * 4 + r != mg)
            def _():
                part = in_ref.at[4 + q, pl.ds(r * 32, 32)]
                pltpu.make_async_remote_copy(
                    src_ref=part,
                    dst_ref=part,
                    send_sem=send.at[32 + q * 4 + r],
                    recv_sem=recv.at[32 + q * 4 + r],
                    device_id=(q * 4 + r, md),
                    device_id_type=pl.DeviceIdType.MESH,
                ).wait_recv()

            return carry

        lax.fori_loop(0, 4, one, 0)

    def spread(product, target, live, total):
        for n in range(8):
            weight = jnp.where((target == n) & live, 1.0, 0.0).astype(F32)
            total[n] += product * weight

    def spread_local(source, total):
        def one(t, carry):
            product = jnp.dot(lt_v[t], source[local_src[0, t]], preferred_element_type=F32)
            spread(product, local_dst[0, t], t < local_count[0], total)
            return carry

        lax.fori_loop(0, 12, one, 0)

    def spread_halo(b, source, total):
        tile = jnp.int32(0)
        for t in range(1, 8):
            tile = jnp.where(halo_src[0, t] == b, t, tile)
        product = jnp.dot(ht_v[tile], source[b], preferred_element_type=F32)
        spread(product, halo_dst[0, tile], tile < 8, total)

    def take_halo(in_ref, send, recv, total):
        def chunk(c, carry):
            off = jnp.where(c == 0, 2, jnp.where(c == 1, 3, jnp.where(c == 2, 1, 0)))
            x = (mx + off) % 4
            q = (mq + off) % 4
            wait_dom(x, in_ref, send, recv)
            spread_halo(x, in_ref, total)
            wait_group(q, in_ref, send, recv)
            spread_halo(4 + q, in_ref, total)
            return carry

        lax.fori_loop(0, 4, chunk, 0)

    def drain(copy_dom, copy_group):
        def one_dom(k, carry):
            d = (md + k) % 32
            copy_dom(d // 8, d % 8).wait_send()
            return carry

        def one_group(k, carry):
            g = (mg + k) % 16
            copy_group(g // 4, g % 4).wait_send()
            return carry

        lax.fori_loop(1, 32, one_dom, 0)
        lax.fori_loop(1, 16, one_group, 0)

    gather_send(enc, 512, out_wide, wide_dom, wide_group)
    keep_own(out_wide, in_wide)

    for n in range(8):
        acc[n] = jnp.broadcast_to(enc_bias[...], (BLK, 512))
        hit = iota((BLK, 256), 0) + n * BLK == remask_nodes[...]
        remasked[n] = jnp.dot(
            jnp.where(hit, 1.0, 0.0).astype(BF16),
            jnp.ones((256, BLK), BF16),
            preferred_element_type=F32,
        )
        acc_thin[n] = jnp.broadcast_to(dec_bias[...], (BLK, BLK))
    masked[...] = jnp.zeros((8, BLK), F32)
    for k in range(4):
        column = jnp.transpose(
            jnp.broadcast_to(mask_nodes[:, k * BLK : (k + 1) * BLK], (BLK, BLK))
        )
        for n in range(8):
            hit = jnp.where(column == iota((BLK, BLK), 1) + n * BLK, 1.0, 0.0)
            masked[n : n + 1] += jnp.sum(hit, axis=0, keepdims=True)

    loads[2].wait()
    loads[3].wait()
    loads[4].wait()
    loads[5].wait()
    spread_local(enc, acc)
    take_halo(in_wide, send_wide, recv_wide, acc)

    def decode(n, carry):
        summed = acc[n]
        latent = jnp.where(summed > 0, summed, enc_slope[...] * summed)
        again = jnp.concatenate([remasked[n]] * 4, axis=1) > 0.5
        decoder_in = jnp.where(again, dec_token[...].astype(F32), latent).astype(BF16)
        narrowed[n] = jnp.dot(decoder_in, decw_v[...], preferred_element_type=F32).astype(BF16)
        return carry

    lax.fori_loop(0, 8, decode, 0)

    gather_send(narrowed, BLK, out_thin, thin_dom, thin_group)
    keep_own(out_thin, in_thin)
    spread_local(narrowed, acc_thin)
    take_halo(in_thin, send_thin, recv_thin, acc_thin)

    ones = jnp.ones((8, BLK), BF16)

    def row_sums(values):
        high = values.astype(BF16)
        low = (values - high.astype(F32)).astype(BF16)
        dims = (((1,), (1,)), ((), ()))
        return lax.dot_general(ones, high, dims, preferred_element_type=F32) + lax.dot_general(
            ones, low, dims, preferred_element_type=F32
        )

    for n in range(8):
        made = acc_thin[n].astype(BF16)
        rebuilt[n] = made
        u = made.astype(F32)
        x = tgt_v[n].astype(F32)
        cosine = (
            row_sums(u * x)
            * (1.0 / BLK)
            * lax.rsqrt(row_sums(u * u) * (1.0 / BLK) + 1e-06)
            * lax.rsqrt(row_sums(x * x) * (1.0 / BLK) + 1e-06)
        )
        error = jnp.where(masked[n : n + 1] > 0.5, (1.0 - cosine[:1]) ** 2, 0.0)
        node_error[n : n + 1] = error

    drain(wide_dom, wide_group)
    drain(thin_dom, thin_group)


def per_device(
    hidden,
    enc_weight,
    enc_bias,
    enc_slope,
    dec_token,
    dec_weight,
    dec_bias,
    targets,
    local_tiles,
    local_src,
    local_dst,
    local_count,
    halo_tiles,
    halo_src,
    halo_dst,
    send_rows,
    cross_rows,
    mask_nodes,
    remask_nodes,
):
    send_index = jnp.concatenate([send_rows.reshape(4, BLK), cross_rows.reshape(4, BLK)], axis=0)
    vmem = pl.BlockSpec(memory_space=pltpu.VMEM)
    smem = pl.BlockSpec(memory_space=pltpu.SMEM)
    far = pl.BlockSpec(memory_space=pl.ANY)
    rebuilt, node_error = pl.pallas_call(
        step_kernel,
        out_shape=(
            jax.ShapeDtypeStruct((8, BLK, BLK), BF16),
            jax.ShapeDtypeStruct((8, BLK), F32),
        ),
        in_specs=[
            far,
            far,
            vmem,
            vmem,
            vmem,
            far,
            vmem,
            far,
            far,
            smem,
            smem,
            smem,
            far,
            smem,
            smem,
            vmem,
            vmem,
            vmem,
        ],
        out_specs=(vmem, vmem),
        scratch_shapes=[
            pltpu.VMEM((8, BLK, 512), BF16),
            pltpu.VMEM((512, 512), BF16),
            pltpu.VMEM((512, BLK), BF16),
            pltpu.VMEM((8, BLK, BLK), BF16),
            pltpu.VMEM((12, BLK, BLK), BF16),
            pltpu.VMEM((8, BLK, BLK), BF16),
            pltpu.VMEM((8, BLK, 512), BF16),
            pltpu.VMEM((8, BLK, 1024), BF16),
            pltpu.VMEM((8, BLK, 512), BF16),
            pltpu.VMEM((8, BLK, 512), BF16),
            pltpu.VMEM((8, BLK, 512), F32),
            pltpu.VMEM((8, BLK, BLK), F32),
            pltpu.VMEM((8, BLK), F32),
            pltpu.VMEM((8, BLK, BLK), BF16),
            pltpu.VMEM((8, BLK, BLK), BF16),
            pltpu.VMEM((8, BLK, BLK), BF16),
            pltpu.VMEM((8, BLK, BLK), F32),
            pltpu.SemaphoreType.DMA((6,)),
            pltpu.SemaphoreType.DMA((48,)),
            pltpu.SemaphoreType.DMA((48,)),
            pltpu.SemaphoreType.DMA((48,)),
            pltpu.SemaphoreType.DMA((48,)),
        ],
        compiler_params=pltpu.CompilerParams(
            collective_id=0, has_side_effects=True, vmem_limit_bytes=56 * 1024 * 1024
        ),
        name="step",
    )(
        hidden.reshape(8, BLK, 512),
        enc_weight,
        enc_bias.reshape(1, 512),
        enc_slope.reshape(1, 512),
        dec_token.reshape(1, 512),
        dec_weight,
        dec_bias.reshape(1, BLK),
        targets.reshape(8, BLK, BLK),
        local_tiles,
        local_src,
        local_dst,
        local_count,
        halo_tiles,
        halo_src,
        halo_dst,
        send_index,
        mask_nodes,
        remask_nodes,
    )
    return rebuilt.reshape(1024, BLK), node_error.reshape(1024)


def solution(mesh):
    both = ("group", "dom")
    in_specs = (
        P(both, None),
        P(),
        P(),
        P(),
        P(),
        P(),
        P(),
        P(both, None),
        P(both, None, None),
        P(both, None),
        P(both, None),
        P(both),
        P(both, None, None),
        P(both, None),
        P(both, None),
        P(both, None),
        P(both, None),
        P(both, None),
        P(both, None),
    )
    out_specs = (P(both, None), P(both))
    return jax.shard_map(
        per_device, mesh=mesh, in_specs=in_specs, out_specs=out_specs, check_vma=False
    )
```

```python
import jax
import jax.numpy as jnp
from jax import lax
from jax.experimental import pallas as pl
from jax.experimental.pallas import tpu as pltpu
from jax.sharding import PartitionSpec as P

BLK = 128
F32 = jnp.float32
BF16 = jnp.bfloat16
I32 = jnp.int32
Z_ORDER = (4, 3, 5, 2, 6, 1, 7, 0)
G_ORDER = (0, 1, 2, 3)


def iota(shape, axis):
    return lax.broadcasted_iota(I32, shape, axis)


def step_kernel(
    hidden,
    enc_weight,
    enc_bias,
    enc_slope,
    dec_token,
    dec_weight,
    dec_bias,
    targets,
    local_tiles,
    local_src,
    local_dst,
    local_count,
    halo_tiles,
    halo_src,
    halo_dst,
    send_rows,
    cross_rows,
    mask_nodes,
    remask_nodes,
    rebuilt,
    node_error,
    hid_v,
    encw_v,
    bias_v,
    slope_v,
    token_v,
    decw_v,
    dbias_v,
    tgt_v,
    lt_v,
    lsrc_s,
    ldst_s,
    ht_v,
    hsrc_s,
    hdst_s,
    send_v,
    cross_v,
    mask_v,
    remask_v,
    square,
    enc,
    onehot,
    out_wide,
    in_wide,
    slots,
    remasked,
    masked,
    norms,
    dots,
    powers,
    narrowed,
    out_thin,
    in_thin,
    slots_thin,
    prev_s,
    final_s,
    tile_s,
    load_sem,
    send_wide,
    recv_wide,
    send_thin,
    recv_thin,
):
    mg = lax.axis_index("group")
    md = lax.axis_index("dom")
    mx = md // 8
    mz = md % 8
    mq = mg // 4

    names = ("send", "cross", "hidden", "encw", "mask", "remask", "lsrc", "ldst")
    names += ("hsrc", "hdst", "bias", "tiles", "tgt", "halo", "slope", "token", "decw", "dbias")
    pairs = (
        (send_rows, send_v),
        (cross_rows, cross_v),
        (hidden, hid_v),
        (enc_weight, encw_v),
        (mask_nodes, mask_v),
        (remask_nodes, remask_v),
        (local_src, lsrc_s),
        (local_dst, ldst_s),
        (halo_src, hsrc_s),
        (halo_dst, hdst_s),
        (enc_bias, bias_v),
        (local_tiles, lt_v),
        (targets, tgt_v),
        (halo_tiles, ht_v),
        (enc_slope, slope_v),
        (dec_token, token_v),
        (dec_weight, decw_v),
        (dec_bias, dbias_v),
    )
    loads = {
        name: pltpu.make_async_copy(src, dst, load_sem.at[k])
        for k, (name, (src, dst)) in enumerate(zip(names, pairs))
    }
    for name in names:
        loads[name].start()

    barrier = pltpu.get_barrier_semaphore()

    def greet_dom(k, carry):
        pl.semaphore_signal(
            barrier, inc=1, device_id=(mg, (md + k) % 32), device_id_type=pl.DeviceIdType.MESH
        )
        return carry

    def greet_group(k, carry):
        pl.semaphore_signal(
            barrier, inc=1, device_id=((mg + k) % 16, md), device_id_type=pl.DeviceIdType.MESH
        )
        return carry

    with jax.named_scope("greet"):
        lax.fori_loop(1, 32, greet_dom, 0)
        lax.fori_loop(1, 16, greet_group, 0)

    def set_rows(row, count, column):
        for j in range(8):
            hit = jnp.broadcast_to(column, (count, BLK)) == iota((count, BLK), 1) + j * BLK
            onehot[row : row + count, j * BLK : (j + 1) * BLK] = jnp.where(hit, 1.0, 0.0).astype(
                BF16
            )

    with jax.named_scope("onehot"):
        loads["send"].wait()
        loads["cross"].wait()
        square[...] = jnp.zeros((BLK, BLK), I32)
        square[0:16, 0:32] = cross_v[...]
        turned = jnp.transpose(square[...])
        for p in range(32):
            set_rows(p * 16, 16, send_v[:, p : p + 1])
        for k in range(16):
            set_rows(512 + k * 32, 32, turned[0:32, k : k + 1])

    with jax.named_scope("load"):
        loads["hidden"].wait()
        loads["encw"].wait()

    def encode(c, carry):
        rows = hid_v[pl.ds(c * 2, 2)].reshape(2 * BLK, 512)
        made = jnp.dot(rows, encw_v[...], preferred_element_type=F32).astype(BF16)
        enc[pl.ds(c * 2, 2)] = made.reshape(2, BLK, 512)
        return carry

    with jax.named_scope("encode"):
        lax.fori_loop(0, 4, encode, 0)

    def dom_copy(out_ref, in_ref, send, recv, d):
        return pltpu.make_async_remote_copy(
            src_ref=out_ref.at[pl.ds(d * 16, 16)],
            dst_ref=in_ref.at[pl.ds(md * 16, 16)],
            send_sem=send,
            recv_sem=recv.at[md],
            device_id=(mg, d),
            device_id_type=pl.DeviceIdType.MESH,
        )

    def group_copy(out_ref, in_ref, send, recv, g):
        return pltpu.make_async_remote_copy(
            src_ref=out_ref.at[pl.ds(512 + g * 32, 32)],
            dst_ref=in_ref.at[pl.ds(512 + mg * 32, 32)],
            send_sem=send,
            recv_sem=recv.at[32 + mg],
            device_id=(g, md),
            device_id_type=pl.DeviceIdType.MESH,
        )

    wide = (out_wide, in_wide, send_wide, recv_wide)
    thin = (out_thin, in_thin, send_thin, recv_thin)

    def push(x, q, ends):
        for k in range(4):
            for z_step in Z_ORDER[2 * k : 2 * k + 2]:
                d = x * 8 + (mz + z_step) % 8

                @pl.when(d != md)
                def _():
                    dom_copy(*ends, d).start()

            g = q * 4 + (mg + G_ORDER[k]) % 4

            @pl.when(g != mg)
            def _():
                group_copy(*ends, g).start()

    def offset(c):
        return jnp.where(c == 0, 2, jnp.where(c == 1, 1, jnp.where(c == 2, 3, 0)))

    def keep_own(out_ref, in_ref):
        own = pl.ds(pl.multiple_of(md * 16, 16), 16)
        in_ref[own] = out_ref[own]
        own = pl.ds(pl.multiple_of(512 + mg * 32, 32), 32)
        in_ref[own] = out_ref[own]

    def wait_dom(x, ends):
        out_ref, in_ref, send, recv = ends

        def one(z, carry):
            d = x * 8 + z

            @pl.when(d != md)
            def _():
                part = in_ref.at[pl.ds(d * 16, 16)]
                pltpu.make_async_remote_copy(
                    src_ref=part,
                    dst_ref=part,
                    send_sem=send,
                    recv_sem=recv.at[d],
                    device_id=(mg, d),
                    device_id_type=pl.DeviceIdType.MESH,
                ).wait_recv()

            return carry

        lax.fori_loop(0, 8, one, 0)

    def wait_group(q, ends):
        out_ref, in_ref, send, recv = ends

        def one(r, carry):
            g = q * 4 + r

            @pl.when(g != mg)
            def _():
                part = in_ref.at[pl.ds(512 + g * 32, 32)]
                pltpu.make_async_remote_copy(
                    src_ref=part,
                    dst_ref=part,
                    send_sem=send,
                    recv_sem=recv.at[32 + g],
                    device_id=(g, md),
                    device_id_type=pl.DeviceIdType.MESH,
                ).wait_recv()

            return carry

        lax.fori_loop(0, 4, one, 0)

    def drain(ends):
        out_ref, in_ref, send, recv = ends
        part = out_ref.at[pl.ds(0, 976)]
        pltpu.make_async_remote_copy(
            src_ref=part,
            dst_ref=part,
            send_sem=send,
            recv_sem=recv.at[0],
            device_id=(mg, md),
            device_id_type=pl.DeviceIdType.MESH,
        ).wait_send()

    def gather_all(c, carry):
        at = pl.ds(pl.multiple_of(c * 256, 256), 256)
        rows = jnp.dot(onehot[at], enc[...].reshape(1024, 512), preferred_element_type=F32)
        out_wide[at] = rows.astype(BF16)
        return carry

    with jax.named_scope("gather_wide"):
        lax.fori_loop(0, 4, gather_all, 0)

    with jax.named_scope("chain"):
        for name in ("lsrc", "ldst", "hsrc", "hdst"):
            loads[name].wait()
        goals = [jnp.where(t < local_count[0], ldst_s[0, t], 8) for t in range(12)]
        for c, off in enumerate((2, 3, 1, 0)):
            for half, b in enumerate(((mx + off) % 4, 4 + (mq + off) % 4)):
                tile = jnp.int32(0)
                for t in range(1, 8):
                    tile = jnp.where(hsrc_s[0, t] == b, t, tile)
                tile_s[2 * c + half] = tile
                goals.append(hdst_s[0, tile])
        for j in range(20):
            prev = jnp.minimum(goals[j], 7)
            for i in range(j):
                prev = jnp.where(goals[i] == goals[j], 8 + i, prev)
            prev_s[j] = prev
        for n in range(8):
            last = jnp.int32(n)
            for i in range(20):
                last = jnp.where(goals[i] == n, 8 + i, last)
            final_s[n] = last

    with jax.named_scope("masks"):
        loads["mask"].wait()
        loads["remask"].wait()
        for n in range(8):
            hit = iota((BLK, 256), 0) + n * BLK == remask_v[...]
            remasked[n] = jnp.dot(
                jnp.where(hit, 1.0, 0.0).astype(BF16),
                jnp.ones((256, BLK), BF16),
                preferred_element_type=F32,
            )
        masked[...] = jnp.zeros((8, BLK), F32)
        for k in range(4):
            column = jnp.transpose(
                jnp.broadcast_to(mask_v[:, k * BLK : (k + 1) * BLK], (BLK, BLK))
            )
            for n in range(8):
                hit = jnp.where(column == iota((BLK, BLK), 1) + n * BLK, 1.0, 0.0)
                masked[n : n + 1] += jnp.sum(hit, axis=0, keepdims=True)

    with jax.named_scope("barrier"):
        pl.semaphore_wait(barrier, 46)

    def push_chunk(c, carry):
        off = offset(c)
        push((mx + off) % 4, (mq + off) % 4, wide)
        return carry

    with jax.named_scope("push"):
        lax.fori_loop(0, 4, push_chunk, 0)
        keep_own(out_wide, in_wide)

    def row_sums(values):
        column = jnp.sum(values, axis=1, keepdims=True)
        on = iota((BLK, BLK), 0) == iota((BLK, BLK), 1)
        return jnp.sum(jnp.where(on, column, 0.0), axis=0, keepdims=True)

    with jax.named_scope("norms"):
        for name in ("bias", "tiles", "tgt", "halo", "slope", "token", "decw", "dbias"):
            loads[name].wait()
        for n in range(8):
            slots[n] = jnp.broadcast_to(bias_v[...], (BLK, 512))
            slots_thin[n] = jnp.broadcast_to(dbias_v[...], (BLK, BLK))
            x = tgt_v[n].astype(F32)
            norms[n : n + 1] = row_sums(x * x)

    def spread_local(source, total):
        def one(t, carry):
            product = jnp.dot(lt_v[t], source[lsrc_s[0, t]], preferred_element_type=F32)
            total[8 + t] = total[prev_s[t]] + product
            return carry

        lax.fori_loop(0, 12, one, 0)

    def take_halo(ends, total):
        in_ref = ends[1]

        def spread(j, b):
            rows = in_ref[pl.ds(pl.multiple_of(b * BLK, BLK), BLK)]
            product = jnp.dot(ht_v[tile_s[j]], rows, preferred_element_type=F32)
            total[20 + j] = total[prev_s[12 + j]] + product

        def chunk(c, carry):
            off = jnp.where(c == 0, 2, jnp.where(c == 1, 3, jnp.where(c == 2, 1, 0)))
            x = (mx + off) % 4
            q = (mq + off) % 4
            with jax.named_scope("wait_dom"):
                wait_dom(x, ends)
            spread(2 * c, x)
            with jax.named_scope("wait_group"):
                wait_group(q, ends)
            spread(2 * c + 1, 4 + q)
            return carry

        lax.fori_loop(0, 4, chunk, 0)

    with jax.named_scope("local_wide"):
        spread_local(enc, slots)
    with jax.named_scope("halo_wide"):
        take_halo(wide, slots)

    token = token_v[...].astype(F32).reshape(1, 512)

    def decode(n, carry):
        summed = slots[final_s[n]]
        latent = jnp.where(summed > 0, summed, slope_v[...] * summed)
        again = jnp.concatenate([remasked[n]] * 4, axis=1) > 0.5
        decoder_in = jnp.where(again, token, latent).astype(BF16)
        narrowed[n] = jnp.dot(decoder_in, decw_v[...], preferred_element_type=F32).astype(BF16)
        return carry

    with jax.named_scope("decode"):
        lax.fori_loop(0, 8, decode, 0)

    def gather_thin(c, carry):
        off = offset(c)
        x = (mx + off) % 4
        q = (mq + off) % 4
        upper = pl.ds(pl.multiple_of(x * BLK, BLK), BLK)
        lower = pl.ds(pl.multiple_of((4 + q) * BLK, BLK), BLK)
        chosen = jnp.concatenate([onehot[upper], onehot[lower]], axis=0)
        rows = jnp.dot(chosen, narrowed[...].reshape(1024, BLK), preferred_element_type=F32)
        rows = rows.astype(BF16)
        out_thin[upper] = rows[:BLK]
        out_thin[lower] = rows[BLK:]
        push(x, q, thin)
        return carry

    with jax.named_scope("gather_thin"):
        lax.fori_loop(0, 4, gather_thin, 0)
        keep_own(out_thin, in_thin)
    with jax.named_scope("local_thin"):
        spread_local(narrowed, slots_thin)
        drain(wide)
    with jax.named_scope("halo_thin"):
        take_halo(thin, slots_thin)

    with jax.named_scope("errors"):
        for n in range(8):
            made = slots_thin[final_s[n]].astype(BF16)
            rebuilt[n] = made
            u = made.astype(F32)
            x = tgt_v[n].astype(F32)
            dots[n : n + 1] = row_sums(u * x)
            powers[n : n + 1] = row_sums(u * u)
        cosine = (
            dots[...]
            * (1.0 / BLK)
            * lax.rsqrt(powers[...] * (1.0 / BLK) + 1e-06)
            * lax.rsqrt(norms[...] * (1.0 / BLK) + 1e-06)
        )
        node_error[...] = jnp.where(masked[...] > 0.5, (1.0 - cosine) ** 2, 0.0)

    with jax.named_scope("drain"):
        drain(thin)


def per_device(
    hidden,
    enc_weight,
    enc_bias,
    enc_slope,
    dec_token,
    dec_weight,
    dec_bias,
    targets,
    local_tiles,
    local_src,
    local_dst,
    local_count,
    halo_tiles,
    halo_src,
    halo_dst,
    send_rows,
    cross_rows,
    mask_nodes,
    remask_nodes,
):
    vmem = pl.BlockSpec(memory_space=pltpu.VMEM)
    smem = pl.BlockSpec(memory_space=pltpu.SMEM)
    far = pl.BlockSpec(memory_space=pl.ANY)
    rebuilt, node_error = pl.pallas_call(
        step_kernel,
        out_shape=(
            pltpu.VMEM((8, BLK, BLK), BF16),
            pltpu.VMEM((8, BLK), F32),
        ),
        in_specs=[far] * 11 + [smem] + [far] * 7,
        out_specs=(vmem, vmem),
        scratch_shapes=[
            pltpu.VMEM((8, BLK, 512), BF16),
            pltpu.VMEM((512, 512), BF16),
            pltpu.VMEM((1, 512), F32),
            pltpu.VMEM((1, 512), F32),
            pltpu.VMEM((512,), BF16),
            pltpu.VMEM((512, BLK), BF16),
            pltpu.VMEM((1, BLK), F32),
            pltpu.VMEM((8, BLK, BLK), BF16),
            pltpu.VMEM((12, BLK, BLK), BF16),
            pltpu.SMEM((1, 12), I32),
            pltpu.SMEM((1, 12), I32),
            pltpu.VMEM((8, BLK, BLK), BF16),
            pltpu.SMEM((1, 8), I32),
            pltpu.SMEM((1, 8), I32),
            pltpu.VMEM((16, 32), I32),
            pltpu.VMEM((16, 32), I32),
            pltpu.VMEM((1, 512), I32),
            pltpu.VMEM((1, 256), I32),
            pltpu.VMEM((BLK, BLK), I32),
            pltpu.VMEM((8, BLK, 512), BF16),
            pltpu.VMEM((1024, 1024), BF16),
            pltpu.VMEM((1024, 512), BF16),
            pltpu.VMEM((1024, 512), BF16),
            pltpu.VMEM((28, BLK, 512), F32),
            pltpu.VMEM((8, BLK, BLK), F32),
            pltpu.VMEM((8, BLK), F32),
            pltpu.VMEM((8, BLK), F32),
            pltpu.VMEM((8, BLK), F32),
            pltpu.VMEM((8, BLK), F32),
            pltpu.VMEM((8, BLK, BLK), BF16),
            pltpu.VMEM((1024, BLK), BF16),
            pltpu.VMEM((1024, BLK), BF16),
            pltpu.VMEM((28, BLK, BLK), F32),
            pltpu.SMEM((20,), I32),
            pltpu.SMEM((8,), I32),
            pltpu.SMEM((8,), I32),
            pltpu.SemaphoreType.DMA((18,)),
            pltpu.SemaphoreType.DMA,
            pltpu.SemaphoreType.DMA((48,)),
            pltpu.SemaphoreType.DMA,
            pltpu.SemaphoreType.DMA((48,)),
        ],
        compiler_params=pltpu.CompilerParams(
            collective_id=0, has_side_effects=True, vmem_limit_bytes=56 * 1024 * 1024
        ),
        name="step",
    )(
        hidden.reshape(8, BLK, 512),
        enc_weight,
        enc_bias.reshape(1, 512),
        enc_slope.reshape(1, 512),
        dec_token,
        dec_weight,
        dec_bias.reshape(1, BLK),
        targets.reshape(8, BLK, BLK),
        local_tiles,
        local_src,
        local_dst,
        local_count,
        halo_tiles,
        halo_src,
        halo_dst,
        send_rows.T,
        cross_rows,
        mask_nodes,
        remask_nodes,
    )
    return rebuilt.reshape(1024, BLK), node_error.reshape(1024)


def solution(mesh):
    both = ("group", "dom")
    in_specs = (
        P(both, None),
        P(),
        P(),
        P(),
        P(),
        P(),
        P(),
        P(both, None),
        P(both, None, None),
        P(both, None),
        P(both, None),
        P(both),
        P(both, None, None),
        P(both, None),
        P(both, None),
        P(both, None),
        P(both, None),
        P(both, None),
        P(both, None),
    )
    out_specs = (P(both, None), P(both))
    return jax.shard_map(
        per_device, mesh=mesh, in_specs=in_specs, out_specs=out_specs, check_vma=False
    )
```

```python
import jax
import jax.numpy as jnp
from jax import lax
from jax.experimental import pallas as pl
from jax.experimental.pallas import tpu as pltpu
from jax.sharding import PartitionSpec as P

BLK = 128
F32 = jnp.float32
BF16 = jnp.bfloat16
I32 = jnp.int32
FAR_X = (2, 1, 3, 0)
FAR_8 = (4, 3, 5, 2, 6, 1, 7, 0)
FAR_DOM = tuple((x, z) for x in FAR_X for z in FAR_8 if x or z)
FAR_GROUP = tuple((y, c) for y in FAR_8 for c in (1, 0) if y or c)


def iota(shape, axis):
    return lax.broadcasted_iota(I32, shape, axis)


def step_kernel(
    hidden,
    enc_weight,
    enc_bias,
    enc_slope,
    dec_token,
    dec_weight,
    dec_bias,
    targets,
    local_tiles,
    local_src,
    local_dst,
    local_count,
    halo_tiles,
    halo_src,
    halo_dst,
    send_rows,
    cross_rows,
    mask_nodes,
    remask_nodes,
    rebuilt,
    node_error,
    hid_v,
    encw_v,
    bias_v,
    slope_v,
    token_v,
    decw_v,
    dbias_v,
    tgt_v,
    lt_v,
    lsrc_s,
    ldst_s,
    lcnt_s,
    ht_v,
    hsrc_s,
    hdst_s,
    send_v,
    cross_v,
    mask_v,
    remask_v,
    square,
    enc,
    onehot,
    out_wide,
    in_wide,
    slots,
    remasked,
    masked,
    norms,
    dots,
    powers,
    narrowed,
    out_thin,
    in_thin,
    slots_thin,
    products,
    prev_s,
    final_s,
    tile_s,
    load_sem,
    send_wide,
    recv_wide,
    send_thin,
    recv_thin,
):
    mg = lax.axis_index("group")
    md = lax.axis_index("dom")
    mx = md // 8
    mz = md % 8
    my = mg // 2
    mc = mg % 2
    mq = mg // 4

    def turn(at, by, size):
        return jnp.where(at + by >= size, at + by - size, at + by)

    xs = [turn(mx, k, 4) for k in range(4)]
    zs = [turn(mz, k, 8) for k in range(8)]
    ys = [turn(my, k, 8) for k in range(8)]
    qs = [turn(mq, k, 4) for k in range(4)]
    cs = [mc, 1 - mc]

    def dom_at(x, z):
        return xs[x] * 8 + zs[z]

    def group_at(y, c):
        return ys[y] * 2 + cs[c]

    names = ("send", "cross", "hidden", "encw", "mask", "remask", "lsrc", "ldst", "lcnt")
    names += ("hsrc", "hdst", "bias", "tiles", "tgt", "halo", "slope", "token", "decw", "dbias")
    pairs = (
        (send_rows, send_v),
        (cross_rows, cross_v),
        (hidden, hid_v),
        (enc_weight, encw_v),
        (mask_nodes, mask_v),
        (remask_nodes, remask_v),
        (local_src, lsrc_s),
        (local_dst, ldst_s),
        (local_count, lcnt_s),
        (halo_src, hsrc_s),
        (halo_dst, hdst_s),
        (enc_bias, bias_v),
        (local_tiles, lt_v),
        (targets, tgt_v),
        (halo_tiles, ht_v),
        (enc_slope, slope_v),
        (dec_token, token_v),
        (dec_weight, decw_v),
        (dec_bias, dbias_v),
    )
    loads = {
        name: pltpu.make_async_copy(src, dst, load_sem.at[k])
        for k, (name, (src, dst)) in enumerate(zip(names, pairs))
    }
    for name in names:
        loads[name].start()

    barrier = pltpu.get_barrier_semaphore()

    with jax.named_scope("greet"):
        for x, z in FAR_DOM:
            pl.semaphore_signal(
                barrier,
                inc=1,
                device_id=(mg, dom_at(x, z)),
                device_id_type=pl.DeviceIdType.MESH,
            )
        for y, c in FAR_GROUP:
            pl.semaphore_signal(
                barrier,
                inc=1,
                device_id=(group_at(y, c), md),
                device_id_type=pl.DeviceIdType.MESH,
            )

    def set_rows(row, count, column):
        for j in range(8):
            hit = jnp.broadcast_to(column, (count, BLK)) == iota((count, BLK), 1) + j * BLK
            onehot[row : row + count, j * BLK : (j + 1) * BLK] = jnp.where(hit, 1.0, 0.0).astype(
                BF16
            )

    with jax.named_scope("onehot"):
        loads["send"].wait()
        loads["cross"].wait()
        square[...] = jnp.zeros((BLK, BLK), I32)
        square[0:16, 0:32] = cross_v[...]
        turned = jnp.transpose(square[...])
        for p in range(32):
            set_rows(p * 16, 16, send_v[:, p : p + 1])
        for k in range(16):
            set_rows(512 + k * 32, 32, turned[0:32, k : k + 1])

    with jax.named_scope("load"):
        loads["hidden"].wait()

    def encode(c, carry):
        rows = hid_v[pl.ds(c * 4, 4)].reshape(4 * BLK, 512)
        made = jnp.dot(rows, encw_v[...], preferred_element_type=F32).astype(BF16)
        enc[pl.ds(c * 4, 4)] = made.reshape(4, BLK, 512)
        return carry

    with jax.named_scope("encode"):
        loads["encw"].wait()
        lax.fori_loop(0, 2, encode, 0)

    def dom_copy(out_ref, in_ref, send, recv, d):
        return pltpu.make_async_remote_copy(
            src_ref=out_ref.at[pl.ds(d * 16, 16)],
            dst_ref=in_ref.at[pl.ds(md * 16, 16)],
            send_sem=send,
            recv_sem=recv,
            device_id=(mg, d),
            device_id_type=pl.DeviceIdType.MESH,
        )

    def group_copy(out_ref, in_ref, send, recv, g):
        return pltpu.make_async_remote_copy(
            src_ref=out_ref.at[pl.ds(512 + g * 32, 32)],
            dst_ref=in_ref.at[pl.ds(512 + mg * 32, 32)],
            send_sem=send,
            recv_sem=recv,
            device_id=(g, md),
            device_id_type=pl.DeviceIdType.MESH,
        )

    wide_dom = (out_wide, in_wide, send_wide, recv_wide.at[mx])
    wide_group = (out_wide, in_wide, send_wide, recv_wide.at[4 + mq])
    thin = (out_thin, in_thin, send_thin, recv_thin)

    def keep_own(out_ref, in_ref):
        own = pl.ds(pl.multiple_of(md * 16, 16), 16)
        in_ref[own] = out_ref[own]
        own = pl.ds(pl.multiple_of(512 + mg * 32, 32), 32)
        in_ref[own] = out_ref[own]

    def await_rows(in_ref, count, send, recv):
        part = in_ref.at[pl.ds(0, count)]
        pltpu.make_async_remote_copy(
            src_ref=part,
            dst_ref=part,
            send_sem=send,
            recv_sem=recv,
            device_id=(mg, md),
            device_id_type=pl.DeviceIdType.MESH,
        ).wait_recv()

    def await_block(b, own, fewer):
        @pl.when(b == own)
        def _():
            await_rows(in_wide, fewer, send_wide, recv_wide.at[b])

        @pl.when(b != own)
        def _():
            await_rows(in_wide, BLK, send_wide, recv_wide.at[b])

    def drain(out_ref, send, recv):
        part = out_ref.at[pl.ds(0, 976)]
        pltpu.make_async_remote_copy(
            src_ref=part,
            dst_ref=part,
            send_sem=send,
            recv_sem=recv,
            device_id=(mg, md),
            device_id_type=pl.DeviceIdType.MESH,
        ).wait_send()

    def gather_all(c, carry):
        at = pl.ds(pl.multiple_of(c * 512, 512), 512)
        rows = jnp.dot(onehot[at], enc[...].reshape(1024, 512), preferred_element_type=F32)
        out_wide[at] = rows.astype(BF16)
        return carry

    with jax.named_scope("gather_wide"):
        lax.fori_loop(0, 2, gather_all, 0)

    with jax.named_scope("barrier"):
        pl.semaphore_wait(barrier, 46)

    with jax.named_scope("push"):
        for k in range(16):
            if k < 15:
                group_copy(*wide_group, group_at(*FAR_GROUP[k])).start()
            for x, z in FAR_DOM[2 * k : 2 * k + 2]:
                dom_copy(*wide_dom, dom_at(x, z)).start()
        keep_own(out_wide, in_wide)

    with jax.named_scope("chain"):
        for name in ("lsrc", "ldst", "lcnt", "hsrc", "hdst"):
            loads[name].wait()
        goals = [jnp.where(t < lcnt_s[0, 0], ldst_s[0, t], 8) for t in range(12)]
        for c, off in enumerate((2, 3, 1, 0)):
            for half, b in enumerate((xs[off], 4 + qs[off])):
                tile = jnp.int32(0)
                for t in range(1, 8):
                    tile = jnp.where(hsrc_s[0, t] == b, t, tile)
                tile_s[2 * c + half] = tile
                goals.append(hdst_s[0, tile])
        for j in range(20):
            prev = jnp.minimum(goals[j], 7)
            for i in range(j):
                prev = jnp.where(goals[i] == goals[j], 8 + i, prev)
            prev_s[j] = prev
        for n in range(8):
            last = jnp.int32(n)
            for i in range(20):
                last = jnp.where(goals[i] == n, 8 + i, last)
            final_s[n] = last

    with jax.named_scope("masks"):
        loads["mask"].wait()
        loads["remask"].wait()
        for n in range(8):
            hit = iota((BLK, 256), 0) + n * BLK == remask_v[...]
            remasked[n] = jnp.dot(
                jnp.where(hit, 1.0, 0.0).astype(BF16),
                jnp.ones((256, BLK), BF16),
                preferred_element_type=F32,
            )
        masked[...] = jnp.zeros((8, BLK), F32)
        for k in range(4):
            column = jnp.transpose(
                jnp.broadcast_to(mask_v[:, k * BLK : (k + 1) * BLK], (BLK, BLK))
            )
            for n in range(8):
                hit = jnp.where(column == iota((BLK, BLK), 1) + n * BLK, 1.0, 0.0)
                masked[n : n + 1] += jnp.sum(hit, axis=0, keepdims=True)

    def row_sums(values):
        column = jnp.sum(values, axis=1, keepdims=True)
        on = iota((BLK, BLK), 0) == iota((BLK, BLK), 1)
        return jnp.sum(jnp.where(on, column, 0.0), axis=0, keepdims=True)

    with jax.named_scope("norms"):
        for name in ("bias", "tiles", "tgt", "halo", "slope", "token", "decw", "dbias"):
            loads[name].wait()
        for n in range(8):
            slots[n] = jnp.broadcast_to(bias_v[...], (BLK, 512))
            slots_thin[n] = jnp.broadcast_to(dbias_v[...], (BLK, BLK))
            x = tgt_v[n].astype(F32)
            norms[n : n + 1] = row_sums(x * x)

    def spread_local(source, total):
        def one(t, carry):
            product = jnp.dot(lt_v[t], source[lsrc_s[0, t]], preferred_element_type=F32)
            total[8 + t] = total[prev_s[t]] + product
            return carry

        lax.fori_loop(0, 12, one, 0)

    def halo_wide(c, carry):
        off = jnp.where(c == 0, 2, jnp.where(c == 1, 3, jnp.where(c == 2, 1, 0)))
        x = (mx + off) % 4
        q = 4 + (mq + off) % 4
        for j, b, own, fewer in ((2 * c, x, mx, 112), (2 * c + 1, q, 4 + mq, 96)):
            with jax.named_scope("await"):
                await_block(b, own, fewer)
            rows = in_wide[pl.ds(pl.multiple_of(b * BLK, BLK), BLK)]
            product = jnp.dot(ht_v[tile_s[j]], rows, preferred_element_type=F32)
            slots[20 + j] = slots[prev_s[12 + j]] + product
        return carry

    with jax.named_scope("local_wide"):
        spread_local(enc, slots)
    with jax.named_scope("halo_wide"):
        lax.fori_loop(0, 4, halo_wide, 0)

    token = token_v[...].astype(F32).reshape(1, 512)

    with jax.named_scope("decode"):
        for n in range(8):
            summed = slots[final_s[n]]
            latent = jnp.where(summed > 0, summed, slope_v[...] * summed)
            again = jnp.concatenate([remasked[n]] * 4, axis=1) > 0.5
            decoder_in = jnp.where(again, token, latent).astype(BF16)
            narrowed[n] = jnp.dot(decoder_in, decw_v[...], preferred_element_type=F32).astype(BF16)

    with jax.named_scope("gather_thin"):
        for x in FAR_X:
            q = qs[x]
            upper = pl.ds(pl.multiple_of(xs[x] * BLK, BLK), BLK)
            lower = pl.ds(pl.multiple_of((4 + q) * BLK, BLK), BLK)
            chosen = jnp.concatenate([onehot[upper], onehot[lower]], axis=0)
            rows = jnp.dot(chosen, narrowed[...].reshape(1024, BLK), preferred_element_type=F32)
            rows = rows.astype(BF16)
            out_thin[upper] = rows[:BLK]
            out_thin[lower] = rows[BLK:]
            for k in range(4):
                for z in FAR_8[2 * k : 2 * k + 2]:
                    if x or z:
                        dom_copy(*thin, dom_at(x, z)).start()
                g = q * 4 + k
                if x:
                    group_copy(*thin, g).start()
                else:

                    @pl.when(g != mg)
                    def _(g=g):
                        group_copy(*thin, g).start()

        keep_own(out_thin, in_thin)
    with jax.named_scope("local_thin"):
        spread_local(narrowed, slots_thin)
        drain(out_wide, send_wide, recv_wide.at[0])
    with jax.named_scope("await_thin"):
        await_rows(in_thin, 976, send_thin, recv_thin)
    with jax.named_scope("halo_thin"):
        for c, off in enumerate((2, 3, 1, 0)):
            for j, b in ((2 * c, xs[off]), (2 * c + 1, 4 + qs[off])):
                rows = in_thin[pl.ds(pl.multiple_of(b * BLK, BLK), BLK)]
                products[j] = jnp.dot(ht_v[tile_s[j]], rows, preferred_element_type=F32)
        for j in range(8):
            slots_thin[20 + j] = slots_thin[prev_s[12 + j]] + products[j]

    with jax.named_scope("errors"):
        for n in range(8):
            made = slots_thin[final_s[n]].astype(BF16)
            rebuilt[n] = made
            u = made.astype(F32)
            x = tgt_v[n].astype(F32)
            dots[n : n + 1] = row_sums(u * x)
            powers[n : n + 1] = row_sums(u * u)
        cosine = (
            dots[...]
            * (1.0 / BLK)
            * lax.rsqrt(powers[...] * (1.0 / BLK) + 1e-06)
            * lax.rsqrt(norms[...] * (1.0 / BLK) + 1e-06)
        )
        node_error[...] = jnp.where(masked[...] > 0.5, (1.0 - cosine) ** 2, 0.0)

    with jax.named_scope("drain"):
        drain(out_thin, send_thin, recv_thin)


def finish_kernel(rebuilt, node_error, rebuilt_out, node_error_out, sem):
    copies = (
        pltpu.make_async_copy(rebuilt, rebuilt_out, sem.at[0]),
        pltpu.make_async_copy(node_error, node_error_out, sem.at[1]),
    )
    for copy in copies:
        copy.start()
    for copy in copies:
        copy.wait()


def per_device(
    hidden,
    enc_weight,
    enc_bias,
    enc_slope,
    dec_token,
    dec_weight,
    dec_bias,
    targets,
    local_tiles,
    local_src,
    local_dst,
    local_count,
    halo_tiles,
    halo_src,
    halo_dst,
    send_rows,
    cross_rows,
    mask_nodes,
    remask_nodes,
):
    vmem = pl.BlockSpec(memory_space=pltpu.VMEM)
    far = pl.BlockSpec(memory_space=pl.ANY)
    rebuilt, node_error = pl.pallas_call(
        step_kernel,
        out_shape=(
            pltpu.VMEM((8, BLK, BLK), BF16),
            pltpu.VMEM((8, BLK), F32),
        ),
        in_specs=[far] * 19,
        out_specs=(vmem, vmem),
        scratch_shapes=[
            pltpu.VMEM((8, BLK, 512), BF16),
            pltpu.VMEM((512, 512), BF16),
            pltpu.VMEM((1, 512), F32),
            pltpu.VMEM((1, 512), F32),
            pltpu.VMEM((512,), BF16),
            pltpu.VMEM((512, BLK), BF16),
            pltpu.VMEM((1, BLK), F32),
            pltpu.VMEM((8, BLK, BLK), BF16),
            pltpu.VMEM((12, BLK, BLK), BF16),
            pltpu.SMEM((1, 12), I32),
            pltpu.SMEM((1, 12), I32),
            pltpu.SMEM((1, 1), I32),
            pltpu.VMEM((8, BLK, BLK), BF16),
            pltpu.SMEM((1, 8), I32),
            pltpu.SMEM((1, 8), I32),
            pltpu.VMEM((16, 32), I32),
            pltpu.VMEM((16, 32), I32),
            pltpu.VMEM((1, 512), I32),
            pltpu.VMEM((1, 256), I32),
            pltpu.VMEM((BLK, BLK), I32),
            pltpu.VMEM((8, BLK, 512), BF16),
            pltpu.VMEM((1024, 1024), BF16),
            pltpu.VMEM((1024, 512), BF16),
            pltpu.VMEM((1024, 512), BF16),
            pltpu.VMEM((28, BLK, 512), F32),
            pltpu.VMEM((8, BLK, BLK), F32),
            pltpu.VMEM((8, BLK), F32),
            pltpu.VMEM((8, BLK), F32),
            pltpu.VMEM((8, BLK), F32),
            pltpu.VMEM((8, BLK), F32),
            pltpu.VMEM((8, BLK, BLK), BF16),
            pltpu.VMEM((1024, BLK), BF16),
            pltpu.VMEM((1024, BLK), BF16),
            pltpu.VMEM((28, BLK, BLK), F32),
            pltpu.VMEM((8, BLK, BLK), F32),
            pltpu.SMEM((20,), I32),
            pltpu.SMEM((8,), I32),
            pltpu.SMEM((8,), I32),
            pltpu.SemaphoreType.DMA((19,)),
            pltpu.SemaphoreType.DMA,
            pltpu.SemaphoreType.DMA((8,)),
            pltpu.SemaphoreType.DMA,
            pltpu.SemaphoreType.DMA,
        ],
        compiler_params=pltpu.CompilerParams(
            collective_id=0, has_side_effects=True, vmem_limit_bytes=56 * 1024 * 1024
        ),
        name="step",
    )(
        hidden.reshape(8, BLK, 512),
        enc_weight,
        enc_bias.reshape(1, 512),
        enc_slope.reshape(1, 512),
        dec_token,
        dec_weight,
        dec_bias.reshape(1, BLK),
        targets.reshape(8, BLK, BLK),
        local_tiles,
        local_src,
        local_dst,
        local_count.reshape(1, 1),
        halo_tiles,
        halo_src,
        halo_dst,
        send_rows.T,
        cross_rows,
        mask_nodes,
        remask_nodes,
    )
    rebuilt, node_error = pl.pallas_call(
        finish_kernel,
        out_shape=(
            jax.ShapeDtypeStruct((8, BLK, BLK), BF16),
            jax.ShapeDtypeStruct((8, BLK), F32),
        ),
        in_specs=[vmem, vmem],
        out_specs=(far, far),
        scratch_shapes=[pltpu.SemaphoreType.DMA((2,))],
        compiler_params=pltpu.CompilerParams(vmem_limit_bytes=4 * 1024 * 1024),
        name="finish",
    )(rebuilt, node_error)
    return rebuilt.reshape(1024, BLK), node_error.reshape(1024)


def solution(mesh):
    both = ("group", "dom")
    in_specs = (
        P(both, None),
        P(),
        P(),
        P(),
        P(),
        P(),
        P(),
        P(both, None),
        P(both, None, None),
        P(both, None),
        P(both, None),
        P(both),
        P(both, None, None),
        P(both, None),
        P(both, None),
        P(both, None),
        P(both, None),
        P(both, None),
        P(both, None),
    )
    out_specs = (P(both, None), P(both))
    return jax.shard_map(
        per_device, mesh=mesh, in_specs=in_specs, out_specs=out_specs, check_vma=False
    )
```

```python
import jax
import jax.numpy as jnp
from jax import lax
from jax.experimental import pallas as pl
from jax.experimental.pallas import tpu as pltpu
from jax.sharding import PartitionSpec as P

BLK = 128
F32 = jnp.float32
BF16 = jnp.bfloat16
I32 = jnp.int32
FAR_X = (2, 1, 3, 0)
FAR_8 = (4, 3, 5, 2, 6, 1, 7, 0)
FAR_DOM = tuple((x, z) for x in FAR_X for z in FAR_8 if x or z)
FAR_GROUP = tuple((y, c) for y in FAR_8 for c in (1, 0) if y or c)


def hops(entry):
    kind, a, b = entry
    if kind == 0:
        return min(a, 4 - a) + min(b, 8 - b)
    return min(a, 8 - a)


GREET = sorted(
    [(0, x, z) for x, z in FAR_DOM] + [(1, y, c) for y, c in FAR_GROUP], key=hops, reverse=True
)


def iota(shape, axis):
    return lax.broadcasted_iota(I32, shape, axis)


def step_kernel(
    hidden,
    enc_weight,
    enc_bias,
    enc_slope,
    dec_token,
    dec_weight,
    dec_bias,
    targets,
    local_tiles,
    local_src,
    local_dst,
    local_count,
    halo_tiles,
    halo_src,
    halo_dst,
    send_rows,
    cross_rows,
    mask_nodes,
    remask_nodes,
    rebuilt,
    node_error,
    hid_v,
    encw_v,
    bias_v,
    slope_v,
    token_v,
    decw_v,
    dbias_v,
    tgt_v,
    lt_v,
    lsrc_s,
    ldst_s,
    lcnt_s,
    ht_v,
    hsrc_s,
    hdst_s,
    send_v,
    cross_v,
    mask_v,
    remask_v,
    square,
    enc,
    onehot,
    out_wide,
    in_wide,
    slots,
    remasked,
    masked,
    norms,
    dots,
    powers,
    narrowed,
    out_thin,
    in_thin,
    slots_thin,
    products,
    prev_s,
    final_s,
    tile_s,
    load_sem,
    send_wide,
    recv_wide,
    send_thin,
    recv_thin,
):
    mg = lax.axis_index("group")
    md = lax.axis_index("dom")
    mx = md // 8
    mz = md % 8
    my = mg // 2
    mc = mg % 2
    mc_y = my % 2
    mq = mg // 4

    def turn(at, by, size):
        return jnp.where(at + by >= size, at + by - size, at + by)

    xs = [turn(mx, k, 4) for k in range(4)]
    zs = [turn(mz, k, 8) for k in range(8)]
    ys = [turn(my, k, 8) for k in range(8)]
    qs = [turn(mq, k, 4) for k in range(4)]
    cs = [mc, 1 - mc]

    def dom_at(x, z):
        return xs[x] * 8 + zs[z]

    def group_at(y, c):
        return ys[y] * 2 + cs[c]

    names = ("send", "cross", "hidden", "encw", "mask", "remask", "lsrc", "ldst", "lcnt")
    names += ("hsrc", "hdst", "bias", "tiles", "tgt", "halo", "slope", "token", "decw", "dbias")
    pairs = (
        (send_rows, send_v),
        (cross_rows, cross_v),
        (hidden, hid_v),
        (enc_weight, encw_v),
        (mask_nodes, mask_v),
        (remask_nodes, remask_v),
        (local_src, lsrc_s),
        (local_dst, ldst_s),
        (local_count, lcnt_s),
        (halo_src, hsrc_s),
        (halo_dst, hdst_s),
        (enc_bias, bias_v),
        (local_tiles, lt_v),
        (targets, tgt_v),
        (halo_tiles, ht_v),
        (enc_slope, slope_v),
        (dec_token, token_v),
        (dec_weight, decw_v),
        (dec_bias, dbias_v),
    )
    loads = {
        name: pltpu.make_async_copy(src, dst, load_sem.at[k])
        for k, (name, (src, dst)) in enumerate(zip(names, pairs))
    }
    for name in names[:4]:
        loads[name].start()

    barrier = pltpu.get_barrier_semaphore()

    with jax.named_scope("greet"):
        for kind, a, b in GREET:
            device = (mg, dom_at(a, b)) if kind == 0 else (group_at(a, b), md)
            pl.semaphore_signal(
                barrier, inc=1, device_id=device, device_id_type=pl.DeviceIdType.MESH
            )

    for name in names[4:]:
        loads[name].start()

    def set_rows(row, count, column):
        for j in range(8):
            hit = jnp.broadcast_to(column, (count, BLK)) == iota((count, BLK), 1) + j * BLK
            onehot[row : row + count, j * BLK : (j + 1) * BLK] = jnp.where(hit, 1.0, 0.0).astype(
                BF16
            )

    with jax.named_scope("onehot"):
        loads["send"].wait()
        loads["cross"].wait()
        square[...] = jnp.zeros((BLK, BLK), I32)
        square[0:16, 0:32] = cross_v[...]
        turned = jnp.transpose(square[...])
        for p in range(32):
            set_rows(p * 16, 16, send_v[:, p : p + 1])
        for k in range(16):
            set_rows(512 + k * 32, 32, turned[0:32, k : k + 1])

    with jax.named_scope("load"):
        loads["hidden"].wait()

    def encode(c, carry):
        rows = hid_v[pl.ds(c * 4, 4)].reshape(4 * BLK, 512)
        made = jnp.dot(rows, encw_v[...], preferred_element_type=F32).astype(BF16)
        enc[pl.ds(c * 4, 4)] = made.reshape(4, BLK, 512)
        return carry

    with jax.named_scope("encode"):
        loads["encw"].wait()
        lax.fori_loop(0, 2, encode, 0)

    def dom_copy(out_ref, in_ref, send, recv, d):
        return pltpu.make_async_remote_copy(
            src_ref=out_ref.at[pl.ds(d * 16, 16)],
            dst_ref=in_ref.at[pl.ds(md * 16, 16)],
            send_sem=send,
            recv_sem=recv,
            device_id=(mg, d),
            device_id_type=pl.DeviceIdType.MESH,
        )

    def group_copy(out_ref, in_ref, send, recv, g):
        return pltpu.make_async_remote_copy(
            src_ref=out_ref.at[pl.ds(512 + g * 32, 32)],
            dst_ref=in_ref.at[pl.ds(512 + mg * 32, 32)],
            send_sem=send,
            recv_sem=recv,
            device_id=(g, md),
            device_id_type=pl.DeviceIdType.MESH,
        )

    wide_dom = (out_wide, in_wide, send_wide, recv_wide.at[mx])
    wide_group = (out_wide, in_wide, send_wide, recv_wide.at[4 + mq])
    thin = (out_thin, in_thin, send_thin, recv_thin)

    def keep_own(out_ref, in_ref):
        own = pl.ds(pl.multiple_of(md * 16, 16), 16)
        in_ref[own] = out_ref[own]
        own = pl.ds(pl.multiple_of(512 + mg * 32, 32), 32)
        in_ref[own] = out_ref[own]

    def await_rows(in_ref, count, send, recv):
        part = in_ref.at[pl.ds(0, count)]
        pltpu.make_async_remote_copy(
            src_ref=part,
            dst_ref=part,
            send_sem=send,
            recv_sem=recv,
            device_id=(mg, md),
            device_id_type=pl.DeviceIdType.MESH,
        ).wait_recv()

    def await_block(b, own, fewer):
        @pl.when(b == own)
        def _():
            await_rows(in_wide, fewer, send_wide, recv_wide.at[b])

        @pl.when(b != own)
        def _():
            await_rows(in_wide, BLK, send_wide, recv_wide.at[b])

    def drain(out_ref, send, recv):
        part = out_ref.at[pl.ds(0, 976)]
        pltpu.make_async_remote_copy(
            src_ref=part,
            dst_ref=part,
            send_sem=send,
            recv_sem=recv,
            device_id=(mg, md),
            device_id_type=pl.DeviceIdType.MESH,
        ).wait_send()

    pair = my + 1 - 2 * mc_y

    def push(dom_ends, group_ends, x):
        groups = [qs[x] * 4 + k for k in range(4)]
        if x == 0:
            groups = [pair * 2, pair * 2 + 1, my * 2 + cs[1]]
        for k in range(4):
            if k < len(groups):
                group_copy(*group_ends, groups[k]).start()
            for z in FAR_8[2 * k : 2 * k + 2]:
                if x or z:
                    dom_copy(*dom_ends, dom_at(x, z)).start()

    def quarter(x):
        upper = pl.ds(pl.multiple_of(xs[x] * BLK, BLK), BLK)
        lower = pl.ds(pl.multiple_of((4 + qs[x]) * BLK, BLK), BLK)
        return upper, lower

    def gather_wide(x):
        upper, lower = quarter(x)
        chosen = jnp.concatenate([onehot[upper], onehot[lower]], axis=0)
        rows = jnp.dot(chosen, enc[...].reshape(1024, 512), preferred_element_type=F32)
        rows = rows.astype(BF16)
        out_wide[upper] = rows[:BLK]
        out_wide[lower] = rows[BLK:]

    with jax.named_scope("gather_wide"):
        gather_wide(FAR_X[0])

    with jax.named_scope("barrier"):
        pl.semaphore_wait(barrier, 46)

    with jax.named_scope("push"):
        for k in range(4):
            push(wide_dom, wide_group, FAR_X[k])
            if k < 3:
                gather_wide(FAR_X[k + 1])
        keep_own(out_wide, in_wide)

    with jax.named_scope("chain"):
        for name in ("lsrc", "ldst", "lcnt", "hsrc", "hdst"):
            loads[name].wait()
        goals = [jnp.where(t < lcnt_s[0, 0], ldst_s[0, t], 8) for t in range(12)]
        for c, off in enumerate((2, 3, 1, 0)):
            for half, b in enumerate((xs[off], 4 + qs[off])):
                tile = jnp.int32(0)
                for t in range(1, 8):
                    tile = jnp.where(hsrc_s[0, t] == b, t, tile)
                tile_s[2 * c + half] = tile
                goals.append(hdst_s[0, tile])
        for j in range(20):
            prev = jnp.minimum(goals[j], 7)
            for i in range(j):
                prev = jnp.where(goals[i] == goals[j], 8 + i, prev)
            prev_s[j] = prev
        for n in range(8):
            last = jnp.int32(n)
            for i in range(20):
                last = jnp.where(goals[i] == n, 8 + i, last)
            final_s[n] = last

    with jax.named_scope("masks"):
        loads["mask"].wait()
        loads["remask"].wait()
        for n in range(8):
            hit = iota((BLK, 256), 0) + n * BLK == remask_v[...]
            remasked[n] = jnp.dot(
                jnp.where(hit, 1.0, 0.0).astype(BF16),
                jnp.ones((256, BLK), BF16),
                preferred_element_type=F32,
            )
        masked[...] = jnp.zeros((8, BLK), F32)
        for k in range(4):
            column = jnp.transpose(
                jnp.broadcast_to(mask_v[:, k * BLK : (k + 1) * BLK], (BLK, BLK))
            )
            for n in range(8):
                hit = jnp.where(column == iota((BLK, BLK), 1) + n * BLK, 1.0, 0.0)
                masked[n : n + 1] += jnp.sum(hit, axis=0, keepdims=True)

    def row_sums(values):
        column = jnp.sum(values, axis=1, keepdims=True)
        on = iota((BLK, BLK), 0) == iota((BLK, BLK), 1)
        return jnp.sum(jnp.where(on, column, 0.0), axis=0, keepdims=True)

    with jax.named_scope("norms"):
        for name in ("bias", "tiles", "tgt", "halo", "slope", "token", "decw", "dbias"):
            loads[name].wait()
        for n in range(8):
            slots[n] = jnp.broadcast_to(bias_v[...], (BLK, 512))
            slots_thin[n] = jnp.broadcast_to(dbias_v[...], (BLK, BLK))
            x = tgt_v[n].astype(F32)
            norms[n : n + 1] = row_sums(x * x)

    def spread_local(source, total):
        def one(t, carry):
            product = jnp.dot(lt_v[t], source[lsrc_s[0, t]], preferred_element_type=F32)
            total[8 + t] = total[prev_s[t]] + product
            return carry

        lax.fori_loop(0, 12, one, 0)

    def halo_wide(c, carry):
        off = jnp.where(c == 0, 2, jnp.where(c == 1, 3, jnp.where(c == 2, 1, 0)))
        x = (mx + off) % 4
        q = 4 + (mq + off) % 4
        for j, b, own, fewer in ((2 * c, x, mx, 112), (2 * c + 1, q, 4 + mq, 96)):
            with jax.named_scope("await"):
                await_block(b, own, fewer)
            rows = in_wide[pl.ds(pl.multiple_of(b * BLK, BLK), BLK)]
            product = jnp.dot(ht_v[tile_s[j]], rows, preferred_element_type=F32)
            slots[20 + j] = slots[prev_s[12 + j]] + product
        return carry

    with jax.named_scope("local_wide"):
        spread_local(enc, slots)
    with jax.named_scope("halo_wide"):
        lax.fori_loop(0, 4, halo_wide, 0)

    token = token_v[...].astype(F32).reshape(1, 512)

    with jax.named_scope("decode"):
        for n in range(8):
            summed = slots[final_s[n]]
            latent = jnp.maximum(summed, slope_v[...] * summed)
            again = jnp.concatenate([remasked[n]] * 4, axis=1) > 0.5
            decoder_in = jnp.where(again, token, latent).astype(BF16)
            narrowed[n] = jnp.dot(decoder_in, decw_v[...], preferred_element_type=F32).astype(BF16)

    with jax.named_scope("gather_thin"):
        waiting = None
        for x in FAR_X:
            upper, lower = quarter(x)
            whole = narrowed[...].reshape(1024, BLK)
            rows = [
                jnp.dot(onehot[span], whole, preferred_element_type=F32) for span in (upper, lower)
            ]
            if waiting is not None:
                push(thin, thin, waiting)
            for span, made in zip((upper, lower), rows):
                out_thin[span] = made.astype(BF16)
            waiting = x
            if x == FAR_X[0]:
                push(thin, thin, x)
                waiting = None
        push(thin, thin, waiting)
        keep_own(out_thin, in_thin)
    with jax.named_scope("local_thin"):
        spread_local(narrowed, slots_thin)
        drain(out_wide, send_wide, recv_wide.at[0])
    with jax.named_scope("await_thin"):
        await_rows(in_thin, 976, send_thin, recv_thin)
    with jax.named_scope("halo_thin"):
        for c, off in enumerate((2, 3, 1, 0)):
            for j, b in ((2 * c, xs[off]), (2 * c + 1, 4 + qs[off])):
                rows = in_thin[pl.ds(pl.multiple_of(b * BLK, BLK), BLK)]
                products[j] = jnp.dot(ht_v[tile_s[j]], rows, preferred_element_type=F32)
        for j in range(8):
            slots_thin[20 + j] = slots_thin[prev_s[12 + j]] + products[j]

    with jax.named_scope("errors"):
        for n in range(8):
            made = slots_thin[final_s[n]].astype(BF16)
            rebuilt[n] = made
            u = made.astype(F32)
            x = tgt_v[n].astype(F32)
            dots[n : n + 1] = row_sums(u * x)
            powers[n : n + 1] = row_sums(u * u)
        cosine = (
            dots[...]
            * (1.0 / BLK)
            * lax.rsqrt(powers[...] * (1.0 / BLK) + 1e-06)
            * lax.rsqrt(norms[...] * (1.0 / BLK) + 1e-06)
        )
        node_error[...] = jnp.where(masked[...] > 0.5, (1.0 - cosine) ** 2, 0.0)

    with jax.named_scope("drain"):
        drain(out_thin, send_thin, recv_thin)


def finish_kernel(rebuilt, node_error, rebuilt_out, node_error_out, sem):
    copies = (
        pltpu.make_async_copy(rebuilt, rebuilt_out, sem.at[0]),
        pltpu.make_async_copy(node_error, node_error_out, sem.at[1]),
    )
    for copy in copies:
        copy.start()
    for copy in copies:
        copy.wait()


def per_device(
    hidden,
    enc_weight,
    enc_bias,
    enc_slope,
    dec_token,
    dec_weight,
    dec_bias,
    targets,
    local_tiles,
    local_src,
    local_dst,
    local_count,
    halo_tiles,
    halo_src,
    halo_dst,
    send_rows,
    cross_rows,
    mask_nodes,
    remask_nodes,
):
    vmem = pl.BlockSpec(memory_space=pltpu.VMEM)
    far = pl.BlockSpec(memory_space=pl.ANY)
    rebuilt, node_error = pl.pallas_call(
        step_kernel,
        out_shape=(
            pltpu.VMEM((8, BLK, BLK), BF16),
            pltpu.VMEM((8, BLK), F32),
        ),
        in_specs=[far] * 19,
        out_specs=(vmem, vmem),
        scratch_shapes=[
            pltpu.VMEM((8, BLK, 512), BF16),
            pltpu.VMEM((512, 512), BF16),
            pltpu.VMEM((1, 512), F32),
            pltpu.VMEM((1, 512), F32),
            pltpu.VMEM((512,), BF16),
            pltpu.VMEM((512, BLK), BF16),
            pltpu.VMEM((1, BLK), F32),
            pltpu.VMEM((8, BLK, BLK), BF16),
            pltpu.VMEM((12, BLK, BLK), BF16),
            pltpu.SMEM((1, 12), I32),
            pltpu.SMEM((1, 12), I32),
            pltpu.SMEM((1, 1), I32),
            pltpu.VMEM((8, BLK, BLK), BF16),
            pltpu.SMEM((1, 8), I32),
            pltpu.SMEM((1, 8), I32),
            pltpu.VMEM((16, 32), I32),
            pltpu.VMEM((16, 32), I32),
            pltpu.VMEM((1, 512), I32),
            pltpu.VMEM((1, 256), I32),
            pltpu.VMEM((BLK, BLK), I32),
            pltpu.VMEM((8, BLK, 512), BF16),
            pltpu.VMEM((1024, 1024), BF16),
            pltpu.VMEM((1024, 512), BF16),
            pltpu.VMEM((1024, 512), BF16),
            pltpu.VMEM((28, BLK, 512), F32),
            pltpu.VMEM((8, BLK, BLK), F32),
            pltpu.VMEM((8, BLK), F32),
            pltpu.VMEM((8, BLK), F32),
            pltpu.VMEM((8, BLK), F32),
            pltpu.VMEM((8, BLK), F32),
            pltpu.VMEM((8, BLK, BLK), BF16),
            pltpu.VMEM((1024, BLK), BF16),
            pltpu.VMEM((1024, BLK), BF16),
            pltpu.VMEM((28, BLK, BLK), F32),
            pltpu.VMEM((8, BLK, BLK), F32),
            pltpu.SMEM((20,), I32),
            pltpu.SMEM((8,), I32),
            pltpu.SMEM((8,), I32),
            pltpu.SemaphoreType.DMA((19,)),
            pltpu.SemaphoreType.DMA,
            pltpu.SemaphoreType.DMA((8,)),
            pltpu.SemaphoreType.DMA,
            pltpu.SemaphoreType.DMA,
        ],
        compiler_params=pltpu.CompilerParams(
            collective_id=0, has_side_effects=True, vmem_limit_bytes=56 * 1024 * 1024
        ),
        name="step",
    )(
        hidden.reshape(8, BLK, 512),
        enc_weight,
        enc_bias.reshape(1, 512),
        enc_slope.reshape(1, 512),
        dec_token,
        dec_weight,
        dec_bias.reshape(1, BLK),
        targets.reshape(8, BLK, BLK),
        local_tiles,
        local_src,
        local_dst,
        local_count.reshape(1, 1),
        halo_tiles,
        halo_src,
        halo_dst,
        send_rows.T,
        cross_rows,
        mask_nodes,
        remask_nodes,
    )
    rebuilt, node_error = pl.pallas_call(
        finish_kernel,
        out_shape=(
            jax.ShapeDtypeStruct((8, BLK, BLK), BF16),
            jax.ShapeDtypeStruct((8, BLK), F32),
        ),
        in_specs=[vmem, vmem],
        out_specs=(far, far),
        scratch_shapes=[pltpu.SemaphoreType.DMA((2,))],
        compiler_params=pltpu.CompilerParams(vmem_limit_bytes=4 * 1024 * 1024),
        name="finish",
    )(rebuilt, node_error)
    return rebuilt.reshape(1024, BLK), node_error.reshape(1024)


def solution(mesh):
    both = ("group", "dom")
    in_specs = (
        P(both, None),
        P(),
        P(),
        P(),
        P(),
        P(),
        P(),
        P(both, None),
        P(both, None, None),
        P(both, None),
        P(both, None),
        P(both),
        P(both, None, None),
        P(both, None),
        P(both, None),
        P(both, None),
        P(both, None),
        P(both, None),
        P(both, None),
    )
    out_specs = (P(both, None), P(both))
    return jax.shard_map(
        per_device, mesh=mesh, in_specs=in_specs, out_specs=out_specs, check_vma=False
    )
```

```python
import jax
import jax.numpy as jnp
from jax import lax
from jax.experimental import pallas as pl
from jax.experimental.pallas import tpu as pltpu
from jax.sharding import PartitionSpec as P

BLK = 128
F32 = jnp.float32
BF16 = jnp.bfloat16
I32 = jnp.int32
FAR_X = (2, 1, 3, 0)
FAR_8 = (4, 3, 5, 2, 6, 1, 7, 0)
FAR_DOM = tuple((x, z) for x in FAR_X for z in FAR_8 if x or z)
FAR_GROUP = tuple((y, c) for y in FAR_8 for c in (1, 0) if y or c)


def hops(entry):
    kind, a, b = entry
    if kind == 0:
        return min(a, 4 - a) + min(b, 8 - b)
    return min(a, 8 - a)


GREET = sorted(
    [(0, x, z) for x, z in FAR_DOM] + [(1, y, c) for y, c in FAR_GROUP], key=hops, reverse=True
)


def iota(shape, axis):
    return lax.broadcasted_iota(I32, shape, axis)


def row_sums(values):
    column = jnp.sum(values, axis=1, keepdims=True)
    on = iota((BLK, BLK), 0) == iota((BLK, BLK), 1)
    return jnp.sum(jnp.where(on, column, 0.0), axis=0, keepdims=True)


def step_kernel(
    hidden,
    enc_weight,
    enc_bias,
    enc_slope,
    dec_token,
    dec_weight,
    dec_bias,
    targets,
    local_tiles,
    local_src,
    local_dst,
    local_count,
    halo_tiles,
    halo_src,
    halo_dst,
    send_rows,
    cross_rows,
    mask_nodes,
    remask_nodes,
    rebuilt,
    tgt_v,
    norms,
    masked,
    hid_v,
    encw_v,
    bias_v,
    slope_v,
    token_v,
    decw_v,
    dbias_v,
    lt_v,
    lsrc_s,
    ldst_s,
    lcnt_s,
    ht_v,
    hsrc_s,
    hdst_s,
    send_v,
    cross_v,
    mask_v,
    remask_v,
    square,
    enc,
    onehot,
    out_wide,
    in_wide,
    slots,
    remasked,
    narrowed,
    out_thin,
    in_thin,
    slots_thin,
    products,
    prev_s,
    final_s,
    tile_s,
    load_sem,
    send_wide,
    recv_wide,
    send_thin,
    recv_thin,
):
    mg = lax.axis_index("group")
    md = lax.axis_index("dom")
    mx = md // 8
    mz = md % 8
    my = mg // 2
    mc = mg % 2
    mc_y = my % 2
    mq = mg // 4

    def turn(at, by, size):
        return jnp.where(at + by >= size, at + by - size, at + by)

    xs = [turn(mx, k, 4) for k in range(4)]
    zs = [turn(mz, k, 8) for k in range(8)]
    ys = [turn(my, k, 8) for k in range(8)]
    qs = [turn(mq, k, 4) for k in range(4)]
    cs = [mc, 1 - mc]

    def dom_at(x, z):
        return xs[x] * 8 + zs[z]

    def group_at(y, c):
        return ys[y] * 2 + cs[c]

    names = ("send", "cross", "hidden", "encw", "mask", "remask", "lsrc", "ldst", "lcnt")
    names += ("hsrc", "hdst", "bias", "tiles", "tgt", "halo", "slope", "token", "decw", "dbias")
    pairs = (
        (send_rows, send_v),
        (cross_rows, cross_v),
        (hidden, hid_v),
        (enc_weight, encw_v),
        (mask_nodes, mask_v),
        (remask_nodes, remask_v),
        (local_src, lsrc_s),
        (local_dst, ldst_s),
        (local_count, lcnt_s),
        (halo_src, hsrc_s),
        (halo_dst, hdst_s),
        (enc_bias, bias_v),
        (local_tiles, lt_v),
        (targets, tgt_v),
        (halo_tiles, ht_v),
        (enc_slope, slope_v),
        (dec_token, token_v),
        (dec_weight, decw_v),
        (dec_bias, dbias_v),
    )
    loads = {
        name: pltpu.make_async_copy(src, dst, load_sem.at[k])
        for k, (name, (src, dst)) in enumerate(zip(names, pairs))
    }
    for name in names[:4]:
        loads[name].start()

    barrier = pltpu.get_barrier_semaphore()

    with jax.named_scope("greet"):
        for kind, a, b in GREET:
            device = (mg, dom_at(a, b)) if kind == 0 else (group_at(a, b), md)
            pl.semaphore_signal(
                barrier, inc=1, device_id=device, device_id_type=pl.DeviceIdType.MESH
            )

    for name in names[4:]:
        loads[name].start()

    def set_rows(row, count, column):
        for j in range(8):
            hit = jnp.broadcast_to(column, (count, BLK)) == iota((count, BLK), 1) + j * BLK
            onehot[row : row + count, j * BLK : (j + 1) * BLK] = jnp.where(hit, 1.0, 0.0).astype(
                BF16
            )

    with jax.named_scope("onehot"):
        loads["send"].wait()
        loads["cross"].wait()
        square[...] = jnp.zeros((BLK, BLK), I32)
        square[0:16, 0:32] = cross_v[...]
        turned = jnp.transpose(square[...])
        for p in range(32):
            set_rows(p * 16, 16, send_v[:, p : p + 1])
        for k in range(16):
            set_rows(512 + k * 32, 32, turned[0:32, k : k + 1])

    with jax.named_scope("load"):
        loads["hidden"].wait()

    def encode(c, carry):
        rows = hid_v[pl.ds(c * 4, 4)].reshape(4 * BLK, 512)
        made = jnp.dot(rows, encw_v[...], preferred_element_type=F32).astype(BF16)
        enc[pl.ds(c * 4, 4)] = made.reshape(4, BLK, 512)
        return carry

    with jax.named_scope("encode"):
        loads["encw"].wait()
        lax.fori_loop(0, 2, encode, 0)

    def dom_copy(out_ref, in_ref, send, recv, d):
        return pltpu.make_async_remote_copy(
            src_ref=out_ref.at[pl.ds(d * 16, 16)],
            dst_ref=in_ref.at[pl.ds(md * 16, 16)],
            send_sem=send,
            recv_sem=recv,
            device_id=(mg, d),
            device_id_type=pl.DeviceIdType.MESH,
        )

    def group_copy(out_ref, in_ref, send, recv, g):
        return pltpu.make_async_remote_copy(
            src_ref=out_ref.at[pl.ds(512 + g * 32, 32)],
            dst_ref=in_ref.at[pl.ds(512 + mg * 32, 32)],
            send_sem=send,
            recv_sem=recv,
            device_id=(g, md),
            device_id_type=pl.DeviceIdType.MESH,
        )

    wide_dom = (out_wide, in_wide, send_wide, recv_wide.at[mx])
    wide_group = (out_wide, in_wide, send_wide, recv_wide.at[4 + mq])
    thin_dom = (out_thin, in_thin, send_thin, recv_thin.at[0])
    thin_group = (out_thin, in_thin, send_thin, recv_thin.at[1])

    def keep_own(out_ref, in_ref):
        own = pl.ds(pl.multiple_of(md * 16, 16), 16)
        in_ref[own] = out_ref[own]
        own = pl.ds(pl.multiple_of(512 + mg * 32, 32), 32)
        in_ref[own] = out_ref[own]

    def await_rows(in_ref, count, send, recv):
        part = in_ref.at[pl.ds(0, count)]
        pltpu.make_async_remote_copy(
            src_ref=part,
            dst_ref=part,
            send_sem=send,
            recv_sem=recv,
            device_id=(mg, md),
            device_id_type=pl.DeviceIdType.MESH,
        ).wait_recv()

    def await_block(b, own, fewer):
        @pl.when(b == own)
        def _():
            await_rows(in_wide, fewer, send_wide, recv_wide.at[b])

        @pl.when(b != own)
        def _():
            await_rows(in_wide, BLK, send_wide, recv_wide.at[b])

    def drain(out_ref, send, recv):
        part = out_ref.at[pl.ds(0, 976)]
        pltpu.make_async_remote_copy(
            src_ref=part,
            dst_ref=part,
            send_sem=send,
            recv_sem=recv,
            device_id=(mg, md),
            device_id_type=pl.DeviceIdType.MESH,
        ).wait_send()

    pair = my + 1 - 2 * mc_y

    def push(dom_ends, group_ends, x):
        groups = [qs[x] * 4 + k for k in range(4)]
        if x == 0:
            groups = [pair * 2, pair * 2 + 1, my * 2 + cs[1]]
        for k in range(4):
            if k < len(groups):
                group_copy(*group_ends, groups[k]).start()
            for z in FAR_8[2 * k : 2 * k + 2]:
                if x or z:
                    dom_copy(*dom_ends, dom_at(x, z)).start()

    def quarter(x):
        upper = pl.ds(pl.multiple_of(xs[x] * BLK, BLK), BLK)
        lower = pl.ds(pl.multiple_of((4 + qs[x]) * BLK, BLK), BLK)
        return upper, lower

    def gather_wide(x):
        upper, lower = quarter(x)
        chosen = jnp.concatenate([onehot[upper], onehot[lower]], axis=0)
        rows = jnp.dot(chosen, enc[...].reshape(1024, 512), preferred_element_type=F32)
        rows = rows.astype(BF16)
        out_wide[upper] = rows[:BLK]
        out_wide[lower] = rows[BLK:]

    with jax.named_scope("gather_wide"):
        gather_wide(FAR_X[0])
        gather_wide(FAR_X[1])

    with jax.named_scope("barrier"):
        pl.semaphore_wait(barrier, 46)

    with jax.named_scope("push"):
        for k in range(4):
            push(wide_dom, wide_group, FAR_X[k])
            if k < 2:
                gather_wide(FAR_X[k + 2])
        keep_own(out_wide, in_wide)

    with jax.named_scope("chain"):
        for name in ("lsrc", "ldst", "lcnt", "hsrc", "hdst"):
            loads[name].wait()
        goals = [jnp.where(t < lcnt_s[0, 0], ldst_s[0, t], 8) for t in range(12)]
        for c, off in enumerate((2, 3, 1, 0)):
            for half, b in enumerate((xs[off], 4 + qs[off])):
                tile = jnp.int32(0)
                for t in range(1, 8):
                    tile = jnp.where(hsrc_s[0, t] == b, t, tile)
                tile_s[2 * c + half] = tile
                goals.append(hdst_s[0, tile])
        for j in range(20):
            prev = jnp.minimum(goals[j], 7)
            for i in range(j):
                prev = jnp.where(goals[i] == goals[j], 8 + i, prev)
            prev_s[j] = prev
        for n in range(8):
            last = jnp.int32(n)
            for i in range(20):
                last = jnp.where(goals[i] == n, 8 + i, last)
            final_s[n] = last

    with jax.named_scope("masks"):
        loads["mask"].wait()
        loads["remask"].wait()
        for n in range(8):
            hit = iota((BLK, 256), 0) + n * BLK == remask_v[...]
            remasked[n] = jnp.dot(
                jnp.where(hit, 1.0, 0.0).astype(BF16),
                jnp.ones((256, BLK), BF16),
                preferred_element_type=F32,
            )
        masked[...] = jnp.zeros((8, BLK), F32)
        for k in range(4):
            column = jnp.transpose(
                jnp.broadcast_to(mask_v[:, k * BLK : (k + 1) * BLK], (BLK, BLK))
            )
            for n in range(8):
                hit = jnp.where(column == iota((BLK, BLK), 1) + n * BLK, 1.0, 0.0)
                masked[n : n + 1] += jnp.sum(hit, axis=0, keepdims=True)

    with jax.named_scope("norms"):
        for name in ("bias", "tiles", "tgt", "halo", "slope", "token", "decw", "dbias"):
            loads[name].wait()
        for n in range(8):
            slots[n] = jnp.broadcast_to(bias_v[...], (BLK, 512))
            slots_thin[n] = jnp.broadcast_to(dbias_v[...], (BLK, BLK))
            x = tgt_v[n].astype(F32)
            norms[n : n + 1] = row_sums(x * x)

    def spread_local(source, total):
        def one(t, carry):
            product = jnp.dot(lt_v[t], source[lsrc_s[0, t]], preferred_element_type=F32)
            total[8 + t] = total[prev_s[t]] + product
            return carry

        lax.fori_loop(0, 12, one, 0)

    def halo_wide(c, carry):
        off = jnp.where(c == 0, 2, jnp.where(c == 1, 3, jnp.where(c == 2, 1, 0)))
        x = (mx + off) % 4
        q = 4 + (mq + off) % 4
        for j, b, own, fewer in ((2 * c, x, mx, 112), (2 * c + 1, q, 4 + mq, 96)):
            with jax.named_scope("await"):
                await_block(b, own, fewer)
            rows = in_wide[pl.ds(pl.multiple_of(b * BLK, BLK), BLK)]
            product = jnp.dot(ht_v[tile_s[j]], rows, preferred_element_type=F32)
            slots[20 + j] = slots[prev_s[12 + j]] + product
        return carry

    with jax.named_scope("local_wide"):
        spread_local(enc, slots)
    with jax.named_scope("halo_wide"):
        lax.fori_loop(0, 4, halo_wide, 0)

    token = token_v[...].astype(F32).reshape(1, 512)

    with jax.named_scope("decode"):
        for n in range(8):
            summed = slots[final_s[n]]
            latent = jnp.maximum(summed, slope_v[...] * summed)
            again = jnp.concatenate([remasked[n]] * 4, axis=1) > 0.5
            decoder_in = jnp.where(again, token, latent).astype(BF16)
            narrowed[n] = jnp.dot(decoder_in, decw_v[...], preferred_element_type=F32).astype(BF16)

    with jax.named_scope("gather_thin"):
        waiting = None
        for x in FAR_X:
            upper, lower = quarter(x)
            whole = narrowed[...].reshape(1024, BLK)
            rows = [
                jnp.dot(onehot[span], whole, preferred_element_type=F32) for span in (upper, lower)
            ]
            if waiting is not None:
                push(thin_dom, thin_group, waiting)
            for span, made in zip((upper, lower), rows):
                out_thin[span] = made.astype(BF16)
            waiting = x
            if x == FAR_X[0]:
                push(thin_dom, thin_group, x)
                waiting = None
        push(thin_dom, thin_group, waiting)
        keep_own(out_thin, in_thin)
    with jax.named_scope("local_thin"):
        spread_local(narrowed, slots_thin)
        drain(out_wide, send_wide, recv_wide.at[0])
    def halo_thin(half):
        for c, off in enumerate((2, 3, 1, 0)):
            b = 4 + qs[off] if half else xs[off]
            rows = in_thin[pl.ds(pl.multiple_of(b * BLK, BLK), BLK)]
            j = 2 * c + half
            products[j] = jnp.dot(ht_v[tile_s[j]], rows, preferred_element_type=F32)

    with jax.named_scope("await_group"):
        await_rows(in_thin, 480, send_thin, recv_thin.at[1])
        halo_thin(1)
    with jax.named_scope("await_thin"):
        await_rows(in_thin, 496, send_thin, recv_thin.at[0])
    with jax.named_scope("halo_thin"):
        halo_thin(0)
        for j in range(8):
            slots_thin[20 + j] = slots_thin[prev_s[12 + j]] + products[j]

    with jax.named_scope("errors"):
        for n in range(8):
            rebuilt[n] = slots_thin[final_s[n]].astype(BF16)

    with jax.named_scope("drain"):
        drain(out_thin, send_thin, recv_thin.at[0])


def finish_kernel(
    rebuilt, targets, norms, masked, rebuilt_out, node_error_out, dots, powers, node_error, sem
):
    values_copy = pltpu.make_async_copy(rebuilt, rebuilt_out, sem.at[0])
    error_copy = pltpu.make_async_copy(node_error, node_error_out, sem.at[1])
    values_copy.start()
    for n in range(8):
        u = rebuilt[n].astype(F32)
        x = targets[n].astype(F32)
        dots[n : n + 1] = row_sums(u * x)
        powers[n : n + 1] = row_sums(u * u)
    cosine = (
        dots[...]
        * (1.0 / BLK)
        * lax.rsqrt(powers[...] * (1.0 / BLK) + 1e-06)
        * lax.rsqrt(norms[...] * (1.0 / BLK) + 1e-06)
    )
    node_error[...] = jnp.where(masked[...] > 0.5, (1.0 - cosine) ** 2, 0.0)
    error_copy.start()
    values_copy.wait()
    error_copy.wait()


def per_device(
    hidden,
    enc_weight,
    enc_bias,
    enc_slope,
    dec_token,
    dec_weight,
    dec_bias,
    targets,
    local_tiles,
    local_src,
    local_dst,
    local_count,
    halo_tiles,
    halo_src,
    halo_dst,
    send_rows,
    cross_rows,
    mask_nodes,
    remask_nodes,
):
    vmem = pl.BlockSpec(memory_space=pltpu.VMEM)
    far = pl.BlockSpec(memory_space=pl.ANY)
    made = pl.pallas_call(
        step_kernel,
        out_shape=(
            pltpu.VMEM((8, BLK, BLK), BF16),
            pltpu.VMEM((8, BLK, BLK), BF16),
            pltpu.VMEM((8, BLK), F32),
            pltpu.VMEM((8, BLK), F32),
        ),
        in_specs=[far] * 19,
        out_specs=(vmem,) * 4,
        scratch_shapes=[
            pltpu.VMEM((8, BLK, 512), BF16),
            pltpu.VMEM((512, 512), BF16),
            pltpu.VMEM((1, 512), F32),
            pltpu.VMEM((1, 512), F32),
            pltpu.VMEM((512,), BF16),
            pltpu.VMEM((512, BLK), BF16),
            pltpu.VMEM((1, BLK), F32),
            pltpu.VMEM((12, BLK, BLK), BF16),
            pltpu.SMEM((1, 12), I32),
            pltpu.SMEM((1, 12), I32),
            pltpu.SMEM((1, 1), I32),
            pltpu.VMEM((8, BLK, BLK), BF16),
            pltpu.SMEM((1, 8), I32),
            pltpu.SMEM((1, 8), I32),
            pltpu.VMEM((16, 32), I32),
            pltpu.VMEM((16, 32), I32),
            pltpu.VMEM((1, 512), I32),
            pltpu.VMEM((1, 256), I32),
            pltpu.VMEM((BLK, BLK), I32),
            pltpu.VMEM((8, BLK, 512), BF16),
            pltpu.VMEM((1024, 1024), BF16),
            pltpu.VMEM((1024, 512), BF16),
            pltpu.VMEM((1024, 512), BF16),
            pltpu.VMEM((28, BLK, 512), F32),
            pltpu.VMEM((8, BLK, BLK), F32),
            pltpu.VMEM((8, BLK, BLK), BF16),
            pltpu.VMEM((1024, BLK), BF16),
            pltpu.VMEM((1024, BLK), BF16),
            pltpu.VMEM((28, BLK, BLK), F32),
            pltpu.VMEM((8, BLK, BLK), F32),
            pltpu.SMEM((20,), I32),
            pltpu.SMEM((8,), I32),
            pltpu.SMEM((8,), I32),
            pltpu.SemaphoreType.DMA((19,)),
            pltpu.SemaphoreType.DMA,
            pltpu.SemaphoreType.DMA((8,)),
            pltpu.SemaphoreType.DMA,
            pltpu.SemaphoreType.DMA((2,)),
        ],
        compiler_params=pltpu.CompilerParams(
            collective_id=0, has_side_effects=True, vmem_limit_bytes=56 * 1024 * 1024
        ),
        name="step",
    )(
        hidden.reshape(8, BLK, 512),
        enc_weight,
        enc_bias.reshape(1, 512),
        enc_slope.reshape(1, 512),
        dec_token,
        dec_weight,
        dec_bias.reshape(1, BLK),
        targets.reshape(8, BLK, BLK),
        local_tiles,
        local_src,
        local_dst,
        local_count.reshape(1, 1),
        halo_tiles,
        halo_src,
        halo_dst,
        send_rows.T,
        cross_rows,
        mask_nodes,
        remask_nodes,
    )
    rebuilt, node_error = pl.pallas_call(
        finish_kernel,
        out_shape=(
            jax.ShapeDtypeStruct((8, BLK, BLK), BF16),
            jax.ShapeDtypeStruct((8, BLK), F32),
        ),
        in_specs=[vmem] * 4,
        out_specs=(far, far),
        scratch_shapes=[
            pltpu.VMEM((8, BLK), F32),
            pltpu.VMEM((8, BLK), F32),
            pltpu.VMEM((8, BLK), F32),
            pltpu.SemaphoreType.DMA((2,)),
        ],
        compiler_params=pltpu.CompilerParams(vmem_limit_bytes=4 * 1024 * 1024),
        name="finish",
    )(*made)
    return rebuilt.reshape(1024, BLK), node_error.reshape(1024)


def solution(mesh):
    both = ("group", "dom")
    in_specs = (
        P(both, None),
        P(),
        P(),
        P(),
        P(),
        P(),
        P(),
        P(both, None),
        P(both, None, None),
        P(both, None),
        P(both, None),
        P(both),
        P(both, None, None),
        P(both, None),
        P(both, None),
        P(both, None),
        P(both, None),
        P(both, None),
        P(both, None),
    )
    out_specs = (P(both, None), P(both))
    return jax.shard_map(
        per_device, mesh=mesh, in_specs=in_specs, out_specs=out_specs, check_vma=False
    )
```
